32 devices in a mesh: slab: 8 (over y, x, core), site: 4 (over z).
Axes of the slice: x: 2, y: 2, z: 4, core: 2. Of those that a mesh axis runs over, the one named last changes fastest.
Arguments:
- potential: float32 [3, 256, 256, 256], P(None, 'slab', 'site'), may hold values from -12 to 12
- t_now: float32 [3, 256, 256, 256], P(None, 'slab', 'site'), may hold values from -3 to 3
- hist_t: float32 [4, 3, 256, 256, 256], P(None, None, 'slab', 'site'), may hold values from -3 to 3
- hist_r: float32 [4, 3, 256, 256, 256], P(None, None, 'slab', 'site'), may hold values from -15 to 15
- chi_self: float32 [3, 256, 256, 256], P(None, ('slab', 'site')), may hold values from 0.3 to 3, as said below
- chi_cross: float32 [3, 256, 256, 256], P(None, ('slab', 'site')), may hold values from -1.8 to 1.8, as said below
Outputs:
- t_next: float32 [3, 256, 256, 256], P(None, 'slab', 'site')
- residual_last: float32 [3, 256, 256, 256], P(None, 'slab', 'site')
The draws below stay inside these ranges and needn't reach their ends.
Inputs may be any that keep to these rules, and one draw needn't show every extreme that they name: `chi_self`: even in the wave vector: the entry at (kx, ky, kz) equals that at (-kx, -ky, -kz), indices taken modulo the grid. `chi_cross`: even in the wave vector: the entry at (kx, ky, kz) equals that at (-kx, -ky, -kz), indices taken modulo the grid.
All inputs are finite; a program needn't handle non-finite values.
Results may differ from the reference program's by a relative error of at most 0.0003.
Values sent between devices are 32-bit elements; how exact they have to be, the bound alone decides.
No kernel may reach another device: no remote copies, remote signals or barrier semaphores. Data moves between devices by JAX's collectives and lax.ppermute only.
A program may use at most 192 MiB of HBM per device.

```python
import math
import jax
import jax.numpy as jnp
import numpy as np
from jax import lax

NX = 256
NY = 256
NZ = 256
SITES = 3
ITERS = 1
HIST = 4
N_SLAB = 8
N_SITE = 4


def wave_order_drawn(depth, devices):
    half_block = depth // (2 * devices)
    rows = np.arange(depth)
    block = rows // (2 * half_block)
    within = rows % (2 * half_block)
    lower = within < half_block
    base = block * half_block + np.where(lower, within, within - half_block)
    partner = np.where(base == 0, depth // 2, depth - base)
    return np.where(lower, base, partner)


def make_even(values):
    mirrored = jnp.roll(jnp.flip(values, (1, 2, 3)), 1, (1, 2, 3))
    even = 0.5 * (values + mirrored)
    order = jnp.asarray(wave_order_drawn(NZ, N_SLAB * N_SITE), jnp.int32)
    return jnp.take(even, order, axis=1)


def position_ramp():
    leading = jnp.arange(NX, dtype=jnp.float32) / (NX - 1)
    trailing = jnp.arange(NY, dtype=jnp.float32) / (NY - 1)
    return 0.5 * (leading[:, None, None] + trailing[None, :, None])


def draw_potential(key, part):
    extent = (SITES, NX, NY, NZ)
    amplitude = jnp.exp(math.log(3.0) * position_ramp())
    values = jnp.clip(jax.random.normal(key, extent, jnp.float32), -4.0, 4.0)
    return values * amplitude[None]


def draw_hist_r(key, part):
    extent = (HIST, SITES, NX, NY, NZ)
    position = position_ramp()[None, None]
    member = jnp.arange(HIST)
    rising = (member % 2 == 0)[:, None, None, None, None]
    amplitude = jnp.exp(math.log(3.0) * jnp.where(rising, position, 1.0 - position))
    own_key = jax.random.fold_in(key, 11)
    values = jnp.clip(jax.random.normal(own_key, extent, jnp.float32), -5.0, 5.0)
    return values * amplitude


def draw_chi_self(key, part):
    extent = (SITES, NZ, NY, NX)
    own_key = jax.random.fold_in(key, 31)
    exponent = jax.random.uniform(own_key, extent, jnp.float32, math.log(0.3), math.log(3.0))
    values = jnp.exp(exponent)
    return make_even(values)


def draw_chi_cross(key, part):
    extent = (SITES, NZ, NY, NX)
    own_key = jax.random.fold_in(key, 47)
    values = 0.3 * jnp.clip(jax.random.normal(own_key, extent, jnp.float32), -6.0, 6.0)
    return make_even(values)


def levels(rng, shape, cuts, low, largest):
    level = 1.0
    for dim, shards_of in cuts:
        steps = jax.random.uniform(jax.random.fold_in(jax.random.fold_in(rng, 6), dim), (shards_of,), jnp.float32, low / len(cuts), largest / len(cuts))
        level = level * jnp.repeat(jnp.exp(steps), shape[dim] // shards_of).reshape((-1,) + (1,) * (len(shape) - 1 - dim))
    return level


def bell_draw(rng, shape, scale, bound, shards=(), kind=jnp.bfloat16):
    loudness = levels(rng, shape, shards, -0.22, 0.18) if shards else 1.0
    entries = jax.random.normal(rng, shape, jnp.float32) * scale * loudness
    return jnp.minimum(jnp.maximum(entries, -bound), bound).astype(kind)


def setup_inputs(seed: int = 0) -> dict:
    splits = jax.random.split(jax.random.key(seed), 7)
    potential = draw_potential(jax.random.fold_in(splits[6], 71), 0)
    t_now = bell_draw(splits[1], (SITES, NX, NY, NZ), 0.5, 3.0, ((1, 8), (2, 4)), jnp.float32)
    hist_t = bell_draw(splits[2], (HIST, SITES, NX, NY, NZ), 0.5, 3.0, ((2, 8), (3, 4)), jnp.float32)
    hist_r = draw_hist_r(jax.random.fold_in(splits[6], 71), 0)
    chi_self = draw_chi_self(jax.random.fold_in(splits[6], 71), 0)
    chi_cross = draw_chi_cross(jax.random.fold_in(splits[6], 71), 0)
    return dict(potential=potential, t_now=t_now, hist_t=hist_t, hist_r=hist_r, chi_self=chi_self, chi_cross=chi_cross)


MIXING = 0.5

def wave_order(depth, devices):
    half_block = depth // (2 * devices)
    rows = np.arange(depth)
    block = rows // (2 * half_block)
    within = rows % (2 * half_block)
    lower = within < half_block
    base = block * half_block + np.where(lower, within, within - half_block)
    partner = np.where(base == 0, depth // 2, depth - base)
    return np.where(lower, base, partner)

def closure(indirect, potential):
    field_value = indirect - potential
    totals = jnp.where(field_value > 0, field_value, jnp.expm1(jnp.minimum(field_value, 0.0)))
    return totals - indirect

def combine_sites(values, self_part, cross_part):
    site_zero, site_one, site_two = (values[0], values[1], values[2])
    out_zero = self_part[0] * site_zero + cross_part[0] * site_one + cross_part[1] * site_two
    out_one = cross_part[0] * site_zero + self_part[1] * site_one + cross_part[2] * site_two
    out_two = cross_part[1] * site_zero + cross_part[2] * site_one + self_part[2] * site_two
    return jnp.stack([out_zero, out_one, out_two])

def residual_of(indirect, potential, self_turned, cross_turned):
    direct_corr = closure(indirect, potential)
    spectrum = jnp.fft.fftn(direct_corr, axes=(1, 2, 3))
    mixed = combine_sites(spectrum, self_turned, cross_turned)
    total_new = jnp.real(jnp.fft.ifftn(mixed, axes=(1, 2, 3))).astype(indirect.dtype)
    return total_new - direct_corr - indirect

def solve_weights(gram):
    count = gram.shape[0]
    factor = [[None] * count for member in range(count)]
    for column in range(count):
        diagonal_sum = gram[column, column]
        for inner in range(column):
            diagonal_sum = diagonal_sum - factor[column][inner] * factor[column][inner]
        factor[column][column] = jnp.sqrt(diagonal_sum)
        for row in range(column + 1, count):
            entry = gram[row, column]
            for inner in range(column):
                entry = entry - factor[row][inner] * factor[column][inner]
            factor[row][column] = entry / factor[column][column]
    middle = []
    for row in range(count):
        entry = jnp.ones((), gram.dtype)
        for inner in range(row):
            entry = entry - factor[row][inner] * middle[inner]
        middle.append(entry / factor[row][row])
    weights = [None] * count
    for row in range(count - 1, -1, -1):
        entry = middle[row]
        for inner in range(row + 1, count):
            entry = entry - factor[inner][row] * weights[inner]
        weights[row] = entry / factor[row][row]
    stacked = jnp.stack(weights)
    return stacked / jnp.sum(stacked)

def extrapolate(iterates, residuals):
    stacked = jnp.stack(residuals).reshape(len(residuals), -1)
    gram = jnp.dot(stacked, stacked.T, precision=lax.Precision.HIGHEST, preferred_element_type=jnp.float32)
    weights = solve_weights(gram)
    result = weights[0] * (iterates[0] + MIXING * residuals[0])
    for member in range(1, len(iterates)):
        result = result + weights[member] * (iterates[member] + MIXING * residuals[member])
    return result

def reference(potential, t_now, hist_t, hist_r, chi_self, chi_cross):
    order = wave_order(NZ, N_SLAB * N_SITE)
    inverse_rows = jnp.asarray(np.argsort(order), jnp.int32)
    self_turned = jnp.transpose(jnp.take(chi_self, inverse_rows, axis=1), (0, 3, 2, 1))
    cross_turned = jnp.transpose(jnp.take(chi_cross, inverse_rows, axis=1), (0, 3, 2, 1))
    iterates = [hist_t[member] for member in range(HIST)]
    residuals = [hist_r[member] for member in range(HIST)]
    indirect = t_now
    latest = t_now
    for iteration in range(ITERS):
        latest = residual_of(indirect, potential, self_turned, cross_turned)
        iterates = iterates + [indirect]
        residuals = residuals + [latest]
        indirect = extrapolate(iterates, residuals)
        iterates = iterates[1:]
        residuals = residuals[1:]
    return (indirect, latest)
```

```python
import functools
import math

import jax
import jax.numpy as jnp
import ml_dtypes
import numpy as np
from jax import lax
from jax.experimental import pallas as pl
from jax.experimental.pallas import tpu as pltpu
from jax.sharding import PartitionSpec as P

MIXING = 0.5
LANES = 128
BOTH = ("slab", "site")
MIB = 1024 * 1024


def halves_of(table):
    high = table.astype(ml_dtypes.bfloat16)
    low = (table - high.astype(np.float64)).astype(ml_dtypes.bfloat16)
    return high, low


def split(values):
    high = values.astype(jnp.bfloat16)
    low = (values - high.astype(jnp.float32)).astype(jnp.bfloat16)
    return high, low


def dot3(left, right, dims):
    dot = functools.partial(
        lax.dot_general, dimension_numbers=(dims, ((), ())), preferred_element_type=jnp.float32
    )
    return dot(left[0], right[0]) + (dot(left[0], right[1]) + dot(left[1], right[0]))


NN = ((1,), (0,))
NT = ((1,), (1,))
TN = ((0,), (0,))


class Plan:
    def __init__(self, mesh, shape):
        self.slabs = mesh.shape["slab"]
        self.sites = mesh.shape["site"]
        self.devices = self.slabs * self.sites
        self.count, self.nx, self.ny, self.nz = shape
        self.rows = self.nx // self.slabs
        self.cols = self.ny // self.sites
        self.pack = LANES // self.cols
        self.planes = self.rows * self.cols // LANES
        self.half = self.nz // (2 * self.devices)
        self.chunks = 2 if self.half % 2 == 0 else 1
        self.per_chunk = self.half // self.chunks
        self.waves = self.devices * self.per_chunk * 2
        self.lines = self.count * self.planes
        self.xblock = min(self.rows, max(1, 1024 // self.cols))

    def depth_tables(self):
        z = np.arange(self.nz)
        forward = np.zeros((self.chunks, self.waves, self.nz))
        inverse = np.zeros((self.chunks, self.waves, self.nz))
        scale = 1.0 / (self.nx * self.ny * self.nz)
        alternate = 1.0 - 2.0 * (z % 2)
        for chunk in range(self.chunks):
            for device in range(self.devices):
                for j in range(self.per_chunk):
                    kz = device * self.half + chunk * self.per_chunk + j
                    row = (device * self.per_chunk + j) * 2
                    angle = 2.0 * math.pi * (kz * z % self.nz) / self.nz
                    if kz == 0:
                        forward[chunk, row] = 1.0
                        forward[chunk, row + 1] = alternate
                        inverse[chunk, row] = scale
                        inverse[chunk, row + 1] = scale * alternate
                    else:
                        forward[chunk, row] = np.cos(angle)
                        forward[chunk, row + 1] = -np.sin(angle)
                        inverse[chunk, row] = 2.0 * scale * np.cos(angle)
                        inverse[chunk, row + 1] = -2.0 * scale * np.sin(angle)
        return forward, inverse

    def plane_tables(self):
        index = np.arange(self.ny)
        angle = 2.0 * math.pi * (index[:, None] * index[None, :] % self.ny) / self.ny
        second = [np.cos(angle), np.sin(angle)]
        low, slab, plane = np.meshgrid(
            np.arange(self.pack), np.arange(self.slabs), np.arange(self.planes), indexing="ij"
        )
        order = (slab * self.rows + plane * self.pack + low).reshape(-1)
        waves = np.arange(self.nx)
        angle = 2.0 * math.pi * (waves[:, None] * order[None, :] % self.nx) / self.nx
        first = [np.cos(angle), np.sin(angle)]
        return second, first, [first[0].T, first[1].T]


def total_of(indirect, potential):
    field_value = indirect - potential
    below = jnp.minimum(field_value, 0.0)
    near = 1.0 / 120.0 + below * (1.0 / 720.0)
    for factor in (1.0 / 24.0, 1.0 / 6.0, 0.5, 1.0):
        near = factor + below * near
    growth = jnp.where(below > -0.25, below * near, jnp.exp(below) - 1.0)
    return jnp.where(field_value > 0, field_value, growth)


def forward_kernel(plan, with_total, t_ref, pot_ref, high_ref, low_ref, *outs):
    out_ref = outs[-1]
    part = pl.program_id(0)
    block = pl.program_id(1)
    size = plan.xblock * plan.cols
    indirect = t_ref[0].reshape(size, plan.nz)
    total = total_of(indirect, pot_ref[0].reshape(size, plan.nz))
    if with_total:
        outs[0][0] = total.reshape(plan.xblock, plan.cols, plan.nz)
    direct = split(total - indirect)
    result = dot3((high_ref[...], low_ref[...]), direct, NT)
    count = size // LANES
    for index in range(count):
        line = part * plan.planes + block * count + index
        out_ref[pl.ds(line, plan.waves, stride=plan.lines), :] = result[
            :, index * LANES : (index + 1) * LANES
        ]


def forward_call(plan, t_now, potential, table, with_total):
    blocks = plan.rows // plan.xblock
    field_spec = pl.BlockSpec(
        (1, plan.xblock, plan.cols, plan.nz), lambda s, b: (s, b, 0, 0)
    )
    table_spec = pl.BlockSpec((plan.waves, plan.nz), lambda s, b: (0, 0))
    rows = plan.waves * plan.lines
    out_specs = [pl.BlockSpec((rows, LANES), lambda s, b: (0, 0))]
    out_shape = [jax.ShapeDtypeStruct((rows, LANES), jnp.float32)]
    if with_total:
        out_specs = [field_spec] + out_specs
        out_shape = [jax.ShapeDtypeStruct(t_now.shape, jnp.float32)] + out_shape
    return pl.pallas_call(
        functools.partial(forward_kernel, plan, with_total),
        grid=(plan.count, blocks),
        in_specs=[field_spec, field_spec, table_spec, table_spec],
        out_specs=out_specs,
        out_shape=out_shape,
        compiler_params=pltpu.CompilerParams(
            dimension_semantics=("arbitrary", "arbitrary"), vmem_limit_bytes=56 * MIB
        ),
        cost_estimate=pl.CostEstimate(
            flops=2 * 3 * t_now.size * plan.waves,
            bytes_accessed=12 * t_now.size,
            transcendentals=t_now.size,
        ),
        name="forward_depth",
    )(t_now, potential, *table)


def middle_kernel(
    plan, first_chunk, in_ref, self_ref, cross_ref, self_top, cross_top, *refs
):
    (tables, rest) = (refs[:12], refs[12:])
    (out_ref, wide, mixed, chi, second) = rest
    step = pl.program_id(0)
    span = plan.slabs * plan.planes
    depth = plan.sites * LANES
    nx, ny = plan.nx, plan.ny
    cols = plan.cols

    @pl.when(step == 0)
    def _():
        second[...] = jnp.zeros_like(second)
        for index in range(4):
            for low in range(plan.pack):
                for site in range(plan.sites):
                    base = site * LANES + low * cols
                    second[index, base : base + cols, low * ny : (low + 1) * ny] = tables[index][
                        site * cols : (site + 1) * cols, :
                    ]

    first_device = jnp.logical_and(lax.axis_index("slab") == 0, lax.axis_index("site") == 0)
    special = jnp.logical_and(first_device, step == 0) if first_chunk else None
    passes = jnp.where(special, 2, 1) if first_chunk else 1

    aligned = plan.planes % 8 == 0

    def repeat(body):
        if aligned:
            lax.fori_loop(0, plan.count, body, 0)
        else:
            for part in range(plan.count):
                body(part, 0)

    def gather(part, imaginary):
        base = (imaginary * plan.count + part) * plan.planes
        base = pl.multiple_of(base, 8) if aligned else base
        pieces = []
        for site in range(plan.sites):
            if aligned:
                piece = in_ref[:, site, 0, pl.ds(base, plan.planes), :].reshape(span, LANES)
            else:
                piece = jnp.concatenate(
                    [
                        in_ref[slab, site, 0, base : base + plan.planes, :]
                        for slab in range(plan.slabs)
                    ],
                    axis=0,
                )
            pieces.append(piece)
        return jnp.concatenate(pieces, axis=1)

    def scatter(part, imaginary, values):
        base = (imaginary * plan.count + part) * plan.planes
        base = pl.multiple_of(base, 8) if aligned else base
        for site in range(plan.sites):
            piece = values[:, site * LANES : (site + 1) * LANES]
            if aligned:
                out_ref[:, site, 0, pl.ds(base, plan.planes), :] = piece.reshape(
                    plan.slabs, plan.planes, LANES
                )
            else:
                for slab in range(plan.slabs):
                    out_ref[slab, site, 0, base : base + plan.planes, :] = piece[
                        slab * plan.planes : (slab + 1) * plan.planes
                    ]

    def run(turn, carry):
        for index in range(plan.count):
            low_self = self_ref[index, 0]
            low_cross = cross_ref[index, 0]
            if first_chunk:
                use_top = turn == 1
                low_self = jnp.where(use_top, self_top[index, 0], low_self)
                low_cross = jnp.where(use_top, cross_top[index, 0], low_cross)
            chi[index] = low_self.T
            chi[plan.count + index] = low_cross.T
        cos_second = (second[0], second[1])
        sin_second = (second[2], second[3])
        cos_first = (tables[4][...], tables[5][...])
        sin_first = (tables[6][...], tables[7][...])
        cos_back = (tables[8][...], tables[9][...])
        sin_back = (tables[10][...], tables[11][...])
        def forward(part, carry):
            real = gather(part, 0)
            imag = gather(part, 1)
            if first_chunk:
                real, imag = (
                    jnp.where(turn == 1, imag, real),
                    jnp.where(special, 0.0, imag),
                )
            real, imag = split(real), split(imag)
            new_real = dot3(real, cos_second, NN) + dot3(imag, sin_second, NN)
            new_imag = dot3(imag, cos_second, NN) - dot3(real, sin_second, NN)
            for low in range(plan.pack):
                wide[low * span : (low + 1) * span, :ny] = new_real[:, low * ny : (low + 1) * ny]
                wide[low * span : (low + 1) * span, ny:] = new_imag[:, low * ny : (low + 1) * ny]
            both = split(wide[...])
            by_cos = dot3(cos_first, both, NN)
            by_sin = dot3(sin_first, both, NN)
            mixed[part, :, :ny] = by_cos[:, :ny] + by_sin[:, ny:]
            mixed[part, :, ny:] = by_cos[:, ny:] - by_sin[:, :ny]
            return carry

        repeat(forward)
        cross_at = {(0, 1): 0, (0, 2): 1, (1, 2): 2}
        strip = 32

        @pl.loop(0, nx // strip)
        def _(index):
            rows = pl.ds(pl.multiple_of(index * strip, strip), strip)
            loaded = [chi[index, rows, :] for index in range(2 * plan.count)]
            for side in range(2):
                lanes = pl.ds(side * ny, ny)
                fields = [mixed[part, rows, lanes] for part in range(plan.count)]
                for part in range(plan.count):
                    value = loaded[part] * fields[part]
                    for other in range(plan.count):
                        if other != part:
                            pair = cross_at[(min(part, other), max(part, other))]
                            value = value + loaded[plan.count + pair] * fields[other]
                    mixed[part, rows, lanes] = value
        def inverse(part, carry):
            both = split(mixed[part])
            by_cos = dot3(cos_back, both, NN)
            by_sin = dot3(sin_back, both, NN)
            real = split(by_cos[:, :ny] - by_sin[:, ny:])
            imag = split(by_cos[:, ny:] + by_sin[:, :ny])
            new_real = None
            new_imag = None
            for low in range(plan.pack):
                rows = slice(low * span, (low + 1) * span)
                lanes = slice(low * ny, (low + 1) * ny)
                cosine = (second[0, :, lanes], second[1, :, lanes])
                sine = (second[2, :, lanes], second[3, :, lanes])
                some_real = (real[0][rows], real[1][rows])
                some_imag = (imag[0][rows], imag[1][rows])
                add_real = dot3(some_real, cosine, NT) - dot3(some_imag, sine, NT)
                add_imag = dot3(some_imag, cosine, NT) + dot3(some_real, sine, NT)
                new_real = add_real if new_real is None else new_real + add_real
                new_imag = add_imag if new_imag is None else new_imag + add_imag
            if first_chunk:

                @pl.when(turn == 0)
                def _(part=part, new_real=new_real):
                    scatter(part, 0, new_real)

                @pl.when(jnp.logical_or(turn == 1, jnp.logical_not(special)))
                def _(part=part, new_real=new_real, new_imag=new_imag):
                    scatter(part, 1, jnp.where(special, new_real, new_imag))
            else:
                scatter(part, 0, new_real)
                scatter(part, 1, new_imag)
            return carry

        repeat(inverse)
        return carry

    if first_chunk:
        lax.fori_loop(0, passes, run, 0)
    else:
        run(0, 0)


def middle_call(plan, chunk, piece, chi_self, chi_cross, tables):
    shape = (plan.slabs, plan.sites, plan.per_chunk, 2 * plan.lines, LANES)
    piece = piece.reshape(shape)
    data_spec = pl.BlockSpec(
        (plan.slabs, plan.sites, 1, 2 * plan.lines, LANES), lambda j: (0, 0, j, 0, 0)
    )
    base = chunk * plan.per_chunk
    row_spec = pl.BlockSpec((plan.count, 1, plan.ny, plan.nx), lambda j: (0, base + j, 0, 0))
    top_spec = pl.BlockSpec((plan.count, 1, plan.ny, plan.nx), lambda j: (0, plan.half, 0, 0))
    table_specs = [pl.BlockSpec(table.shape, lambda j: (0, 0)) for table in tables]
    depth = plan.sites * LANES
    flops = 2 * 3 * 2 * plan.count * 4 * plan.per_chunk * plan.nx * plan.ny * (plan.nx + depth)
    return pl.pallas_call(
        functools.partial(middle_kernel, plan, chunk == 0),
        grid=(plan.per_chunk,),
        in_specs=[data_spec, row_spec, row_spec, top_spec, top_spec] + table_specs,
        out_specs=data_spec,
        out_shape=jax.ShapeDtypeStruct(shape, jnp.float32),
        scratch_shapes=[
            pltpu.VMEM((plan.nx, 2 * plan.ny), jnp.float32),
            pltpu.VMEM((plan.count, plan.nx, 2 * plan.ny), jnp.float32),
            pltpu.VMEM((2 * plan.count, plan.nx, plan.ny), jnp.float32),
            pltpu.VMEM((4, depth, plan.pack * plan.ny), jnp.bfloat16),
        ],
        compiler_params=pltpu.CompilerParams(
            dimension_semantics=("arbitrary",), vmem_limit_bytes=56 * MIB
        ),
        cost_estimate=pl.CostEstimate(
            flops=flops, bytes_accessed=4 * piece.size * 4, transcendentals=0
        ),
        name="middle_planes",
    )(piece, chi_self, chi_cross, chi_self, chi_cross, *tables)


def fold(values):
    return jnp.sum(values.reshape(-1, 8, values.shape[-1]), axis=0)


def history_kernel(plan, members, t_ref, r_ref, u_ref, sum_ref):
    first = jnp.logical_and(pl.program_id(0) == 0, pl.program_id(1) == 0)

    @pl.when(first)
    def _():
        sum_ref[...] = jnp.zeros_like(sum_ref)

    residuals = [r_ref[member, 0] for member in range(members)]
    for member in range(members):
        u_ref[member, 0] = t_ref[member, 0] + MIXING * residuals[member]
    index = 0
    for i in range(members):
        for j in range(i + 1):
            sum_ref[index] += fold(residuals[i] * residuals[j])
            index += 1


def history_call(plan, hist_t, hist_r):
    members = hist_t.shape[0]
    block = (members, 1, min(plan.xblock, 4), plan.cols, plan.nz)
    spec = pl.BlockSpec(block, lambda s, b: (0, s, b, 0, 0))
    pairs = members * (members + 1) // 2
    sum_spec = pl.BlockSpec((pairs, 8, plan.nz), lambda s, b: (0, 0, 0))
    return pl.pallas_call(
        functools.partial(history_kernel, plan, members),
        grid=(plan.count, plan.rows // block[2]),
        in_specs=[spec, spec],
        out_specs=[spec, sum_spec],
        out_shape=[
            jax.ShapeDtypeStruct(hist_t.shape, jnp.float32),
            jax.ShapeDtypeStruct((pairs, 8, plan.nz), jnp.float32),
        ],
        compiler_params=pltpu.CompilerParams(
            dimension_semantics=("arbitrary", "arbitrary"), vmem_limit_bytes=56 * MIB
        ),
        cost_estimate=pl.CostEstimate(
            flops=50 * hist_t.size, bytes_accessed=12 * hist_t.size, transcendentals=0
        ),
        name="history",
    )(hist_t, hist_r)


def residual_kernel(plan, members, *refs):
    pieces = refs[: plan.chunks]
    (high_ref, low_ref, total_ref, r_ref, old_ref, out_ref, stat_ref, acc) = refs[plan.chunks :]
    part = pl.program_id(0)
    block = pl.program_id(1)
    first = jnp.logical_and(part == 0, block == 0)
    last = jnp.logical_and(part == pl.num_programs(0) - 1, block == pl.num_programs(1) - 1)

    @pl.when(first)
    def _():
        acc[...] = jnp.zeros_like(acc)

    size = plan.xblock * plan.cols
    count = size // LANES
    for index in range(count):
        line = part * plan.planes + block * count + index
        gathered = jnp.concatenate(
            [piece[pl.ds(line, plan.waves, stride=plan.lines), :] for piece in pieces], axis=0
        )
        turned = split(gathered.T)
        field = dot3(turned, (high_ref[...], low_ref[...]), NN)
        rows = pl.ds(index * plan.pack, plan.pack)
        field = field.reshape(plan.pack, plan.cols, plan.nz) - total_ref[0, rows]
        out_ref[0, rows] = field
        for member in range(members):
            acc[member] += fold(field * r_ref[member, 0, rows])
        acc[members] += fold(field * field)

    @pl.when(last)
    def _():
        lane = lax.broadcasted_iota(jnp.int32, (8, LANES), 1)
        stats = jnp.zeros((8, LANES), jnp.float32)
        pairs = members * (members + 1) // 2
        for index in range(pairs + members + 1):
            tile = old_ref[index] if index < pairs else acc[index - pairs]
            stats = jnp.where(lane == index, jnp.sum(tile), stats)
        stat_ref[...] = stats


def residual_call(plan, pieces, table, total, hist_r, old_sums):
    members = hist_r.shape[0]
    rows = plan.waves * plan.lines
    pieces = [piece.reshape(rows, LANES) for piece in pieces]
    spec = pl.BlockSpec((1, plan.xblock, plan.cols, plan.nz), lambda s, b: (s, b, 0, 0))
    hist_spec = pl.BlockSpec(
        (members, 1, plan.xblock, plan.cols, plan.nz), lambda s, b: (0, s, b, 0, 0)
    )
    whole = lambda array: pl.BlockSpec(array.shape, lambda s, b: (0,) * array.ndim)
    return pl.pallas_call(
        functools.partial(residual_kernel, plan, members),
        grid=(plan.count, plan.rows // plan.xblock),
        in_specs=[whole(piece) for piece in pieces]
        + [whole(table[0]), whole(table[1]), spec, hist_spec, whole(old_sums)],
        out_specs=[spec, pl.BlockSpec((8, LANES), lambda s, b: (0, 0))],
        out_shape=[
            jax.ShapeDtypeStruct(total.shape, jnp.float32),
            jax.ShapeDtypeStruct((8, LANES), jnp.float32),
        ],
        scratch_shapes=[pltpu.VMEM((members + 1, 8, plan.nz), jnp.float32)],
        compiler_params=pltpu.CompilerParams(
            dimension_semantics=("arbitrary", "arbitrary"), vmem_limit_bytes=56 * MIB
        ),
        cost_estimate=pl.CostEstimate(
            flops=2 * 3 * total.size * plan.nz,
            bytes_accessed=4 * total.size * (3 + members),
            transcendentals=0,
        ),
        name="residual",
    )(*pieces, *table, total, hist_r, old_sums)


def solve_weights(gram, count):
    factor = [[None] * count for member in range(count)]
    for column in range(count):
        diagonal_sum = gram[column][column]
        for inner in range(column):
            diagonal_sum = diagonal_sum - factor[column][inner] * factor[column][inner]
        factor[column][column] = jnp.sqrt(diagonal_sum)
        for row in range(column + 1, count):
            entry = gram[row][column]
            for inner in range(column):
                entry = entry - factor[row][inner] * factor[column][inner]
            factor[row][column] = entry / factor[column][column]
    middle = []
    for row in range(count):
        entry = jnp.ones_like(gram[0][0])
        for inner in range(row):
            entry = entry - factor[row][inner] * middle[inner]
        middle.append(entry / factor[row][row])
    weights = [None] * count
    for row in range(count - 1, -1, -1):
        entry = middle[row]
        for inner in range(row + 1, count):
            entry = entry - factor[inner][row] * weights[inner]
        weights[row] = entry / factor[row][row]
    whole = weights[0]
    for row in range(1, count):
        whole = whole + weights[row]
    return [weight / whole for weight in weights]


def combine_kernel(plan, members, stat_ref, u_ref, t_ref, res_ref, out_ref, weight_ref):
    first = jnp.logical_and(pl.program_id(0) == 0, pl.program_id(1) == 0)

    @pl.when(first)
    def _():
        stats = jnp.sum(stat_ref[...], axis=0)
        lane = lax.broadcasted_iota(jnp.int32, (8, LANES), 1)
        gram = []
        index = 0
        for i in range(members + 1):
            row = []
            for j in range(i + 1):
                chosen = jnp.where(lane == index, stats, 0.0)
                row.append(jnp.sum(chosen, axis=1, keepdims=True))
                index += 1
            gram.append(row)
        weights = solve_weights(gram, members + 1)
        for member in range(members + 1):
            weight_ref[member] = jnp.broadcast_to(weights[member], (8, LANES))

    weights = [weight_ref[member, 0:1, 0:1] for member in range(members + 1)]
    value = weights[members] * (t_ref[0] + MIXING * res_ref[0])
    for member in range(members):
        value = value + weights[member] * u_ref[member, 0]
    out_ref[0] = value


def combine_call(plan, stats, mixed_history, t_now, residual):
    members = mixed_history.shape[0]
    rows = plan.xblock
    spec = pl.BlockSpec((1, rows, plan.cols, plan.nz), lambda s, b: (s, b, 0, 0))
    hist_spec = pl.BlockSpec((members, 1, rows, plan.cols, plan.nz), lambda s, b: (0, s, b, 0, 0))
    return pl.pallas_call(
        functools.partial(combine_kernel, plan, members),
        grid=(plan.count, plan.rows // rows),
        in_specs=[pl.BlockSpec(stats.shape, lambda s, b: (0, 0, 0)), hist_spec, spec, spec],
        out_specs=spec,
        out_shape=jax.ShapeDtypeStruct(t_now.shape, jnp.float32),
        scratch_shapes=[pltpu.VMEM((members + 1, 8, LANES), jnp.float32)],
        compiler_params=pltpu.CompilerParams(
            dimension_semantics=("arbitrary", "arbitrary"), vmem_limit_bytes=56 * MIB
        ),
        cost_estimate=pl.CostEstimate(
            flops=10 * t_now.size, bytes_accessed=4 * t_now.size * (members + 3), transcendentals=0
        ),
        name="combine",
    )(stats, mixed_history, t_now, residual)


def exchange(array):
    return lax.all_to_all(array, BOTH, split_axis=0, concat_axis=0, tiled=True)


def local(plan, potential, t_now, hist_t, hist_r, chi_self, chi_cross):
    forward, inverse = plan.depth_tables()
    plane_tables = []
    for group in plan.plane_tables():
        for table in group:
            plane_tables.extend(jnp.asarray(half) for half in halves_of(table))
    inverse = halves_of(inverse.reshape(plan.chunks * plan.waves, plan.nz))
    inverse = [jnp.asarray(half) for half in inverse]
    shape = (plan.devices, plan.per_chunk * 2 * plan.lines, LANES)
    sent = []
    total = None
    for chunk in range(plan.chunks):
        table = [jnp.asarray(half) for half in halves_of(forward[chunk])]
        with_total = chunk == plan.chunks - 1
        outs = forward_call(plan, t_now, potential, table, with_total)
        if with_total:
            total = outs[0]
        sent.append(exchange(outs[-1].reshape(shape)))
    mixed_history, old_sums = history_call(plan, hist_t, hist_r)
    back = []
    for chunk in range(plan.chunks):
        planes = middle_call(plan, chunk, sent[chunk], chi_self, chi_cross, plane_tables)
        back.append(exchange(planes.reshape(shape)))
    residual, stats = residual_call(plan, back, inverse, total, hist_r, old_sums)
    copies = jnp.broadcast_to(stats, (plan.devices,) + stats.shape)
    gathered = exchange(copies)
    result = combine_call(plan, gathered, mixed_history, t_now, residual)
    return (result, residual)


def solution(mesh):
    def body(potential, t_now, hist_t, hist_r, chi_self, chi_cross):
        shape = (
            t_now.shape[0],
            t_now.shape[1] * mesh.shape["slab"],
            t_now.shape[2] * mesh.shape["site"],
            t_now.shape[3],
        )
        return local(Plan(mesh, shape), potential, t_now, hist_t, hist_r, chi_self, chi_cross)

    return jax.shard_map(
        body,
        mesh=mesh,
        in_specs=(
            P(None, "slab", "site", None),
            P(None, "slab", "site", None),
            P(None, None, "slab", "site", None),
            P(None, None, "slab", "site", None),
            P(None, BOTH, None, None),
            P(None, BOTH, None, None),
        ),
        out_specs=(P(None, "slab", "site", None), P(None, "slab", "site", None)),
        check_vma=False,
    )
```

```python
import functools
import math

import jax
import jax.numpy as jnp
import ml_dtypes
import numpy as np
from jax import lax
from jax.experimental import pallas as pl
from jax.experimental.pallas import tpu as pltpu
from jax.sharding import PartitionSpec as P

MIXING = 0.5
LANES = 128
BOTH = ("slab", "site")
MIB = 1024 * 1024
SPLITS = 4


def halves_of(table):
    high = table.astype(ml_dtypes.bfloat16)
    low = (table - high.astype(np.float64)).astype(ml_dtypes.bfloat16)
    return high, low


def split(values):
    high = values.astype(jnp.bfloat16)
    low = (values - high.astype(jnp.float32)).astype(jnp.bfloat16)
    return high, low


def dot3(left, right, dims):
    dot = functools.partial(
        lax.dot_general, dimension_numbers=(dims, ((), ())), preferred_element_type=jnp.float32
    )
    return dot(left[0], right[0]) + (dot(left[0], right[1]) + dot(left[1], right[0]))


NN = ((1,), (0,))
NT = ((1,), (1,))
TN = ((0,), (0,))


class Plan:
    def __init__(self, mesh, shape):
        self.slabs = mesh.shape["slab"]
        self.sites = mesh.shape["site"]
        self.devices = self.slabs * self.sites
        self.count, self.nx, self.ny, self.nz = shape
        self.rows = self.nx // self.slabs
        self.cols = self.ny // self.sites
        self.pack = LANES // self.cols
        self.planes = self.rows * self.cols // LANES
        self.half = self.nz // (2 * self.devices)
        self.chunks = 2 if self.half % 2 == 0 else 1
        self.per_chunk = self.half // self.chunks
        self.waves = self.devices * self.per_chunk * 2
        self.lines = self.count * self.planes
        self.xblock = min(self.rows, max(1, 1024 // self.cols))

    def depth_tables(self):
        z = np.arange(self.nz)
        forward = np.zeros((self.chunks, self.waves, self.nz))
        inverse = np.zeros((self.chunks, self.waves, self.nz))
        scale = 1.0 / (self.nx * self.ny * self.nz)
        alternate = 1.0 - 2.0 * (z % 2)
        for chunk in range(self.chunks):
            for device in range(self.devices):
                for j in range(self.per_chunk):
                    kz = device * self.half + chunk * self.per_chunk + j
                    row = (device * self.per_chunk + j) * 2
                    angle = 2.0 * math.pi * (kz * z % self.nz) / self.nz
                    if kz == 0:
                        forward[chunk, row] = 1.0
                        forward[chunk, row + 1] = alternate
                        inverse[chunk, row] = scale
                        inverse[chunk, row + 1] = scale * alternate
                    else:
                        forward[chunk, row] = np.cos(angle)
                        forward[chunk, row + 1] = -np.sin(angle)
                        inverse[chunk, row] = 2.0 * scale * np.cos(angle)
                        inverse[chunk, row + 1] = -2.0 * scale * np.sin(angle)
        return forward, inverse

    def plane_tables(self):
        index = np.arange(self.ny)
        angle = 2.0 * math.pi * (index[:, None] * index[None, :] % self.ny) / self.ny
        second = [np.cos(angle), np.sin(angle)]
        low, slab, plane = np.meshgrid(
            np.arange(self.pack), np.arange(self.slabs), np.arange(self.planes), indexing="ij"
        )
        order = (slab * self.rows + plane * self.pack + low).reshape(-1)
        waves = np.arange(self.nx)
        angle = 2.0 * math.pi * (waves[:, None] * order[None, :] % self.nx) / self.nx
        first = [np.cos(angle), np.sin(angle)]
        return second, first, [first[0].T, first[1].T]


def total_of(indirect, potential):
    field_value = indirect - potential
    near = field_value + field_value * field_value * (0.5 + field_value * (1.0 / 6.0))
    growth = jnp.where(field_value > -0.01, near, jnp.exp(field_value) - 1.0)
    return jnp.where(field_value > 0, field_value, growth)


def forward_kernel(plan, with_total, t_ref, pot_ref, high_ref, low_ref, *refs):
    outs = refs[-2:] if with_total else refs[-1:]
    out_ref = outs[-1]
    part = pl.program_id(0)
    block = pl.program_id(1)
    size = plan.xblock * plan.cols
    indirect = t_ref[0].reshape(size, plan.nz)
    total = total_of(indirect, pot_ref[0].reshape(size, plan.nz))
    if with_total:
        outs[0][0] = total.reshape(plan.xblock, plan.cols, plan.nz)
    direct = split(total - indirect)
    result = dot3((high_ref[...], low_ref[...]), direct, NT)
    count = size // LANES
    for index in range(count):
        line = part * plan.planes + block * count + index
        out_ref[pl.ds(line, plan.waves, stride=plan.lines), :] = result[
            :, index * LANES : (index + 1) * LANES
        ]


def forward_call(plan, t_now, potential, table, with_total, tokens):
    blocks = plan.rows // plan.xblock
    field_spec = pl.BlockSpec(
        (1, plan.xblock, plan.cols, plan.nz), lambda s, b: (s, b, 0, 0)
    )
    table_spec = pl.BlockSpec((plan.waves, plan.nz), lambda s, b: (0, 0))
    rows = plan.waves * plan.lines
    out_specs = [pl.BlockSpec((rows, LANES), lambda s, b: (0, 0))]
    out_shape = [jax.ShapeDtypeStruct((rows, LANES), jnp.float32)]
    if with_total:
        out_specs = [field_spec] + out_specs
        out_shape = [jax.ShapeDtypeStruct(t_now.shape, jnp.float32)] + out_shape
    return pl.pallas_call(
        functools.partial(forward_kernel, plan, with_total),
        grid=(plan.count, blocks),
        in_specs=[field_spec, field_spec, table_spec, table_spec]
        + [pl.BlockSpec(memory_space=pl.ANY)] * len(tokens),
        out_specs=out_specs,
        out_shape=out_shape,
        compiler_params=pltpu.CompilerParams(
            dimension_semantics=("arbitrary", "arbitrary"), vmem_limit_bytes=56 * MIB
        ),
        cost_estimate=pl.CostEstimate(
            flops=2 * 3 * t_now.size * plan.waves,
            bytes_accessed=12 * t_now.size,
            transcendentals=t_now.size,
        ),
        name="forward_depth",
    )(t_now, potential, *table, *tokens)


def middle_kernel(
    plan, first_chunk, in_ref, self_ref, cross_ref, self_top, cross_top, *refs
):
    (tables, rest) = (refs[:12], refs[12:])
    (out_ref, wide, mixed, chi, second) = rest
    step = pl.program_id(0)
    span = plan.slabs * plan.planes
    depth = plan.sites * LANES
    nx, ny = plan.nx, plan.ny
    cols = plan.cols

    @pl.when(step == 0)
    def _():
        second[...] = jnp.zeros_like(second)
        for index in range(4):
            for low in range(plan.pack):
                for site in range(plan.sites):
                    base = site * LANES + low * cols
                    second[index, base : base + cols, low * ny : (low + 1) * ny] = tables[index][
                        site * cols : (site + 1) * cols, :
                    ]

    first_device = jnp.logical_and(lax.axis_index("slab") == 0, lax.axis_index("site") == 0)
    special = jnp.logical_and(first_device, step == 0) if first_chunk else None
    passes = jnp.where(special, 2, 1) if first_chunk else 1

    aligned = plan.planes % 8 == 0

    def repeat(body):
        if aligned:
            lax.fori_loop(0, plan.count, body, 0)
        else:
            for part in range(plan.count):
                body(part, 0)

    def gather(part, imaginary):
        base = (imaginary * plan.count + part) * plan.planes
        base = pl.multiple_of(base, 8) if aligned else base
        pieces = []
        for site in range(plan.sites):
            if aligned:
                piece = in_ref[:, site, 0, pl.ds(base, plan.planes), :].reshape(span, LANES)
            else:
                piece = jnp.concatenate(
                    [
                        in_ref[slab, site, 0, base : base + plan.planes, :]
                        for slab in range(plan.slabs)
                    ],
                    axis=0,
                )
            pieces.append(piece)
        return jnp.concatenate(pieces, axis=1)

    def scatter(part, imaginary, values):
        base = (imaginary * plan.count + part) * plan.planes
        base = pl.multiple_of(base, 8) if aligned else base
        for site in range(plan.sites):
            piece = values[:, site * LANES : (site + 1) * LANES]
            if aligned:
                out_ref[:, site, 0, pl.ds(base, plan.planes), :] = piece.reshape(
                    plan.slabs, plan.planes, LANES
                )
            else:
                for slab in range(plan.slabs):
                    out_ref[slab, site, 0, base : base + plan.planes, :] = piece[
                        slab * plan.planes : (slab + 1) * plan.planes
                    ]

    def run(turn, carry):
        for index in range(plan.count):
            low_self = self_ref[index, 0]
            low_cross = cross_ref[index, 0]
            if first_chunk:
                use_top = turn == 1
                low_self = jnp.where(use_top, self_top[index, 0], low_self)
                low_cross = jnp.where(use_top, cross_top[index, 0], low_cross)
            chi[index] = low_self.T
            chi[plan.count + index] = low_cross.T
        cos_second = (second[0], second[1])
        sin_second = (second[2], second[3])
        cos_first = (tables[4][...], tables[5][...])
        sin_first = (tables[6][...], tables[7][...])
        cos_back = (tables[8][...], tables[9][...])
        sin_back = (tables[10][...], tables[11][...])
        def forward(part, carry):
            real = gather(part, 0)
            imag = gather(part, 1)
            if first_chunk:
                real, imag = (
                    jnp.where(turn == 1, imag, real),
                    jnp.where(special, 0.0, imag),
                )
            real, imag = split(real), split(imag)
            new_real = dot3(real, cos_second, NN) + dot3(imag, sin_second, NN)
            new_imag = dot3(imag, cos_second, NN) - dot3(real, sin_second, NN)
            for low in range(plan.pack):
                wide[low * span : (low + 1) * span, :ny] = new_real[:, low * ny : (low + 1) * ny]
                wide[low * span : (low + 1) * span, ny:] = new_imag[:, low * ny : (low + 1) * ny]
            both = split(wide[...])
            by_cos = dot3(cos_first, both, NN)
            by_sin = dot3(sin_first, both, NN)
            mixed[part, :, :ny] = by_cos[:, :ny] + by_sin[:, ny:]
            mixed[part, :, ny:] = by_cos[:, ny:] - by_sin[:, :ny]
            return carry

        repeat(forward)
        cross_at = {(0, 1): 0, (0, 2): 1, (1, 2): 2}
        strip = 32

        @pl.loop(0, nx // strip)
        def _(index):
            rows = pl.ds(pl.multiple_of(index * strip, strip), strip)
            loaded = [chi[index, rows, :] for index in range(2 * plan.count)]
            for side in range(2):
                lanes = pl.ds(side * ny, ny)
                fields = [mixed[part, rows, lanes] for part in range(plan.count)]
                for part in range(plan.count):
                    value = loaded[part] * fields[part]
                    for other in range(plan.count):
                        if other != part:
                            pair = cross_at[(min(part, other), max(part, other))]
                            value = value + loaded[plan.count + pair] * fields[other]
                    mixed[part, rows, lanes] = value
        def inverse(part, carry):
            both = split(mixed[part])
            by_cos = dot3(cos_back, both, NN)
            by_sin = dot3(sin_back, both, NN)
            real = split(by_cos[:, :ny] - by_sin[:, ny:])
            imag = split(by_cos[:, ny:] + by_sin[:, :ny])
            new_real = None
            new_imag = None
            for low in range(plan.pack):
                rows = slice(low * span, (low + 1) * span)
                lanes = slice(low * ny, (low + 1) * ny)
                cosine = (second[0, :, lanes], second[1, :, lanes])
                sine = (second[2, :, lanes], second[3, :, lanes])
                some_real = (real[0][rows], real[1][rows])
                some_imag = (imag[0][rows], imag[1][rows])
                add_real = dot3(some_real, cosine, NT) - dot3(some_imag, sine, NT)
                add_imag = dot3(some_imag, cosine, NT) + dot3(some_real, sine, NT)
                new_real = add_real if new_real is None else new_real + add_real
                new_imag = add_imag if new_imag is None else new_imag + add_imag
            if first_chunk:

                @pl.when(turn == 0)
                def _(part=part, new_real=new_real):
                    scatter(part, 0, new_real)

                @pl.when(jnp.logical_or(turn == 1, jnp.logical_not(special)))
                def _(part=part, new_real=new_real, new_imag=new_imag):
                    scatter(part, 1, jnp.where(special, new_real, new_imag))
            else:
                scatter(part, 0, new_real)
                scatter(part, 1, new_imag)
            return carry

        repeat(inverse)
        return carry

    if first_chunk:
        lax.fori_loop(0, passes, run, 0)
    else:
        run(0, 0)


def middle_call(plan, chunk, piece, chi_self, chi_cross, tables):
    shape = (plan.slabs, plan.sites, plan.per_chunk, 2 * plan.lines, LANES)
    piece = piece.reshape(shape)
    if chunk < plan.chunks - 1:
        piece = pltpu.with_memory_space_constraint(piece, pltpu.VMEM)
    data_spec = pl.BlockSpec(
        (plan.slabs, plan.sites, 1, 2 * plan.lines, LANES), lambda j: (0, 0, j, 0, 0)
    )
    base = chunk * plan.per_chunk
    row_spec = pl.BlockSpec((plan.count, 1, plan.ny, plan.nx), lambda j: (0, base + j, 0, 0))
    top_spec = pl.BlockSpec((plan.count, 1, plan.ny, plan.nx), lambda j: (0, plan.half, 0, 0))
    table_specs = [pl.BlockSpec(table.shape, lambda j: (0, 0)) for table in tables]
    depth = plan.sites * LANES
    flops = 2 * 3 * 2 * plan.count * 4 * plan.per_chunk * plan.nx * plan.ny * (plan.nx + depth)
    return pl.pallas_call(
        functools.partial(middle_kernel, plan, chunk == 0),
        grid=(plan.per_chunk,),
        in_specs=[data_spec, row_spec, row_spec, top_spec, top_spec]
        + table_specs,
        out_specs=data_spec,
        out_shape=jax.ShapeDtypeStruct(shape, jnp.float32),
        scratch_shapes=[
            pltpu.VMEM((plan.nx, 2 * plan.ny), jnp.float32),
            pltpu.VMEM((plan.count, plan.nx, 2 * plan.ny), jnp.float32),
            pltpu.VMEM((2 * plan.count, plan.nx, plan.ny), jnp.float32),
            pltpu.VMEM((4, depth, plan.pack * plan.ny), jnp.bfloat16),
        ],
        compiler_params=pltpu.CompilerParams(
            dimension_semantics=("arbitrary",), vmem_limit_bytes=56 * MIB
        ),
        cost_estimate=pl.CostEstimate(
            flops=flops, bytes_accessed=4 * piece.size * 4, transcendentals=0
        ),
        name="middle_planes",
    )(piece, chi_self, chi_cross, chi_self, chi_cross, *tables)


def fold(values):
    return jnp.sum(values.reshape(-1, 8, values.shape[-1]), axis=0)


def history_kernel(plan, members, t_ref, r_ref, u_ref, sum_ref):
    first = jnp.logical_and(pl.program_id(0) == 0, pl.program_id(1) == 0)

    @pl.when(first)
    def _():
        sum_ref[...] = jnp.zeros_like(sum_ref)

    residuals = [r_ref[member, 0] for member in range(members)]
    for member in range(members):
        u_ref[member, 0] = t_ref[member, 0] + MIXING * residuals[member]
    index = 0
    for i in range(members):
        for j in range(i + 1):
            sum_ref[index] += fold(residuals[i] * residuals[j])
            index += 1


def history_call(plan, hist_t, hist_r):
    members = hist_t.shape[0]
    block = (members, 1, min(plan.xblock, 4), plan.cols, plan.nz)
    spec = pl.BlockSpec(block, lambda s, b: (0, s, b, 0, 0))
    pairs = members * (members + 1) // 2
    sum_spec = pl.BlockSpec((pairs, 8, plan.nz), lambda s, b: (0, 0, 0))
    return pl.pallas_call(
        functools.partial(history_kernel, plan, members),
        grid=(plan.count, plan.rows // block[2]),
        in_specs=[spec, spec],
        out_specs=[spec, sum_spec],
        out_shape=[
            pltpu.HBM(hist_t.shape, jnp.float32),
            jax.ShapeDtypeStruct((pairs, 8, plan.nz), jnp.float32),
        ],
        compiler_params=pltpu.CompilerParams(
            dimension_semantics=("arbitrary", "arbitrary"), vmem_limit_bytes=56 * MIB
        ),
        cost_estimate=pl.CostEstimate(
            flops=50 * hist_t.size, bytes_accessed=12 * hist_t.size, transcendentals=0
        ),
        name="history",
    )(hist_t, hist_r)


def residual_kernel(plan, members, *refs):
    pieces = refs[: plan.chunks]
    (high_ref, low_ref, total_ref, r_ref, old_ref, out_ref, stat_ref, acc) = refs[plan.chunks :]
    part = pl.program_id(0)
    block = pl.program_id(1)
    first = jnp.logical_and(part == 0, block == 0)
    last = jnp.logical_and(part == pl.num_programs(0) - 1, block == pl.num_programs(1) - 1)

    @pl.when(first)
    def _():
        acc[...] = jnp.zeros_like(acc)

    size = plan.xblock * plan.cols
    count = size // LANES
    for index in range(count):
        line = part * plan.planes + block * count + index
        gathered = jnp.concatenate(
            [piece[pl.ds(line, plan.waves, stride=plan.lines), :] for piece in pieces], axis=0
        )
        turned = split(gathered.T)
        field = dot3(turned, (high_ref[...], low_ref[...]), NN)
        rows = pl.ds(index * plan.pack, plan.pack)
        field = field.reshape(plan.pack, plan.cols, plan.nz) - total_ref[0, rows]
        out_ref[0, rows] = field
        for member in range(members):
            acc[member] += fold(field * r_ref[member, 0, rows])
        acc[members] += fold(field * field)

    @pl.when(last)
    def _():
        lane = lax.broadcasted_iota(jnp.int32, (8, LANES), 1)
        stats = jnp.zeros((8, LANES), jnp.float32)
        pairs = members * (members + 1) // 2
        for index in range(pairs + members + 1):
            tile = old_ref[index] if index < pairs else acc[index - pairs]
            stats = jnp.where(lane == index, jnp.sum(tile), stats)
        stat_ref[...] = stats


def residual_call(plan, pieces, table, total, hist_r, old_sums):
    members = hist_r.shape[0]
    rows = plan.waves * plan.lines
    pieces = [in_hbm(piece.reshape(rows, LANES)) for piece in pieces]
    spec = pl.BlockSpec((1, plan.xblock, plan.cols, plan.nz), lambda s, b: (s, b, 0, 0))
    hist_spec = pl.BlockSpec(
        (members, 1, plan.xblock, plan.cols, plan.nz), lambda s, b: (0, s, b, 0, 0)
    )
    whole = lambda array: pl.BlockSpec(array.shape, lambda s, b: (0,) * array.ndim)
    return pl.pallas_call(
        functools.partial(residual_kernel, plan, members),
        grid=(plan.count, plan.rows // plan.xblock),
        in_specs=[whole(piece) for piece in pieces]
        + [whole(table[0]), whole(table[1]), spec, hist_spec, whole(old_sums)],
        out_specs=[spec, pl.BlockSpec((8, LANES), lambda s, b: (0, 0))],
        out_shape=[
            pltpu.HBM(total.shape, jnp.float32),
            jax.ShapeDtypeStruct((8, LANES), jnp.float32),
        ],
        scratch_shapes=[pltpu.VMEM((members + 1, 8, plan.nz), jnp.float32)],
        compiler_params=pltpu.CompilerParams(
            dimension_semantics=("arbitrary", "arbitrary"), vmem_limit_bytes=56 * MIB
        ),
        cost_estimate=pl.CostEstimate(
            flops=2 * 3 * total.size * plan.nz,
            bytes_accessed=4 * total.size * (3 + members),
            transcendentals=0,
        ),
        name="residual",
    )(*pieces, *table, total, hist_r, old_sums)


def dual_kernel(plan, r_ref, high_ref, low_ref, out_ref):
    part = pl.program_id(1)
    block = pl.program_id(2)
    size = plan.xblock * plan.cols
    values = split(r_ref[0, 0].reshape(size, plan.nz))
    result = dot3((high_ref[...], low_ref[...]), values, NT)
    count = size // LANES
    for index in range(count):
        line = part * plan.planes + block * count + index
        out_ref[0, pl.ds(line, plan.waves, stride=plan.lines), :] = result[
            :, index * LANES : (index + 1) * LANES
        ]


def dual_call(plan, hist_r, table):
    members = hist_r.shape[0]
    rows = plan.waves * plan.lines
    spec = pl.BlockSpec(
        (1, 1, plan.xblock, plan.cols, plan.nz), lambda m, s, b: (m, s, b, 0, 0)
    )
    table_spec = pl.BlockSpec((plan.waves, plan.nz), lambda m, s, b: (0, 0))
    return pl.pallas_call(
        functools.partial(dual_kernel, plan),
        grid=(members, plan.count, plan.rows // plan.xblock),
        in_specs=[spec, table_spec, table_spec],
        out_specs=pl.BlockSpec((1, rows, LANES), lambda m, s, b: (m, 0, 0)),
        out_shape=jax.ShapeDtypeStruct((members, rows, LANES), jnp.float32),
        compiler_params=pltpu.CompilerParams(
            dimension_semantics=("arbitrary",) * 3, vmem_limit_bytes=56 * MIB
        ),
        cost_estimate=pl.CostEstimate(
            flops=2 * 3 * hist_r.size * plan.waves,
            bytes_accessed=6 * hist_r.size,
            transcendentals=0,
        ),
        name="dual",
    )(hist_r, *table)


def partial_kernel(plan, members, *refs):
    pieces = refs[: plan.chunks - 1]
    (high_ref, low_ref, total_ref, r_ref, out_ref, acc) = refs[plan.chunks - 1 :]
    part = pl.program_id(0)
    block = pl.program_id(1)

    @pl.when(jnp.logical_and(part == 0, block == 0))
    def _():
        acc[...] = jnp.zeros_like(acc)

    count = plan.xblock * plan.cols // LANES
    for index in range(count):
        field, rows = piece_field(plan, pieces, high_ref, low_ref, index)
        field = field - total_ref[0, rows]
        out_ref[0, rows] = field
        for member in range(members):
            acc[member] += fold(field * r_ref[member, 0, rows])


def piece_field(plan, pieces, high_ref, low_ref, index):
    count = plan.xblock * plan.cols // LANES
    line = pl.program_id(0) * plan.planes + pl.program_id(1) * count + index
    gathered = [piece[pl.ds(line, plan.waves, stride=plan.lines), :] for piece in pieces]
    gathered = gathered[0] if len(gathered) == 1 else jnp.concatenate(gathered, axis=0)
    field = dot3(split(gathered.T), (high_ref[...], low_ref[...]), NN)
    rows = pl.ds(index * plan.pack, plan.pack)
    return field.reshape(plan.pack, plan.cols, plan.nz), rows


def partial_call(plan, pieces, table, total, hist_r):
    members = hist_r.shape[0]
    rows = plan.waves * plan.lines
    pieces = [in_hbm(piece.reshape(rows, LANES)) for piece in pieces]
    spec = pl.BlockSpec((1, plan.xblock, plan.cols, plan.nz), lambda s, b: (s, b, 0, 0))
    hist_spec = pl.BlockSpec(
        (members, 1, plan.xblock, plan.cols, plan.nz), lambda s, b: (0, s, b, 0, 0)
    )
    whole = lambda array: pl.BlockSpec(array.shape, lambda s, b: (0,) * array.ndim)
    return pl.pallas_call(
        functools.partial(partial_kernel, plan, members),
        grid=(plan.count, plan.rows // plan.xblock),
        in_specs=[whole(array) for array in (*pieces, *table)] + [spec, hist_spec],
        out_specs=[spec, pl.BlockSpec((members, 8, plan.nz), lambda s, b: (0, 0, 0))],
        out_shape=[
            jax.ShapeDtypeStruct(total.shape, jnp.float32),
            jax.ShapeDtypeStruct((members, 8, plan.nz), jnp.float32),
        ],
        compiler_params=pltpu.CompilerParams(
            dimension_semantics=("arbitrary", "arbitrary"), vmem_limit_bytes=56 * MIB
        ),
        cost_estimate=pl.CostEstimate(
            flops=2 * 3 * total.size * plan.nz,
            bytes_accessed=4 * total.size * (3 + members),
            transcendentals=0,
        ),
        name="partial",
    )(*pieces, *table, total, hist_r)


def final_kernel(plan, members, *refs):
    (piece_ref, high_ref, low_ref, base_ref, dual_ref, old_ref, some_ref) = refs[:7]
    (out_ref, stat_ref, keep_ref, acc, square) = refs[7:]
    part = pl.program_id(0)
    block = pl.program_id(1)
    blocks = pl.num_programs(1)
    first = jnp.logical_and(part == 0, block == 0)
    last = jnp.logical_and(part == pl.num_programs(0) - 1, block == blocks - 1)

    @pl.when(first)
    def _():
        acc[...] = jnp.zeros_like(acc)
        square[...] = jnp.zeros_like(square)

    share = dual_ref.shape[1]
    start = pl.multiple_of((part * blocks + block) * share, share)
    waves = piece_ref[pl.ds(start, share), :]
    for member in range(members):
        acc[member] += fold(waves * dual_ref[member])
    count = plan.xblock * plan.cols // LANES
    for index in range(count):
        field, rows = piece_field(plan, [piece_ref], high_ref, low_ref, index)
        field = field + base_ref[0, rows]
        out_ref[0, rows] = field
        keep_ref[part, pl.ds(block * plan.xblock + index * plan.pack, plan.pack)] = field
        square[...] += fold(field * field)

    @pl.when(last)
    def _():
        lane = lax.broadcasted_iota(jnp.int32, (8, LANES), 1)
        stats = jnp.zeros((8, LANES), jnp.float32)
        pairs = members * (members + 1) // 2
        for index in range(pairs):
            stats = jnp.where(lane == index, jnp.sum(old_ref[index]), stats)
        for member in range(members):
            value = jnp.sum(some_ref[member]) + jnp.sum(acc[member])
            stats = jnp.where(lane == pairs + member, value, stats)
        stats = jnp.where(lane == pairs + members, jnp.sum(square[...]), stats)
        stat_ref[...] = stats


def final_call(plan, piece, table, base, duals, old_sums, some_sums):
    members = duals.shape[0]
    rows = plan.waves * plan.lines
    piece = in_hbm(piece.reshape(rows, LANES))
    blocks = plan.rows // plan.xblock
    share = rows // (plan.count * blocks)
    spec = pl.BlockSpec((1, plan.xblock, plan.cols, plan.nz), lambda s, b: (s, b, 0, 0))
    dual_spec = pl.BlockSpec((members, share, LANES), lambda s, b: (0, s * blocks + b, 0))
    whole = lambda array: pl.BlockSpec(array.shape, lambda s, b: (0,) * array.ndim)
    return pl.pallas_call(
        functools.partial(final_kernel, plan, members),
        grid=(plan.count, blocks),
        in_specs=[whole(piece), whole(table[0]), whole(table[1]), spec, dual_spec]
        + [whole(old_sums), whole(some_sums)],
        out_specs=[
            spec,
            pl.BlockSpec((8, LANES), lambda s, b: (0, 0)),
            pl.BlockSpec(memory_space=pltpu.VMEM),
        ],
        out_shape=[
            jax.ShapeDtypeStruct(base.shape, jnp.float32),
            jax.ShapeDtypeStruct((8, LANES), jnp.float32),
            pltpu.VMEM(base.shape, jnp.float32),
        ],
        scratch_shapes=[
            pltpu.VMEM((members, 8, LANES), jnp.float32),
            pltpu.VMEM((8, plan.nz), jnp.float32),
        ],
        compiler_params=pltpu.CompilerParams(
            dimension_semantics=("arbitrary", "arbitrary"), vmem_limit_bytes=50 * MIB
        ),
        cost_estimate=pl.CostEstimate(
            flops=2 * 3 * base.size * plan.waves,
            bytes_accessed=4 * base.size * 5,
            transcendentals=0,
        ),
        name="final",
    )(piece, *table, base, duals, old_sums, some_sums)


def solve_weights(gram, count):
    factor = [[None] * count for member in range(count)]
    for column in range(count):
        diagonal_sum = gram[column][column]
        for inner in range(column):
            diagonal_sum = diagonal_sum - factor[column][inner] * factor[column][inner]
        factor[column][column] = jnp.sqrt(diagonal_sum)
        for row in range(column + 1, count):
            entry = gram[row][column]
            for inner in range(column):
                entry = entry - factor[row][inner] * factor[column][inner]
            factor[row][column] = entry / factor[column][column]
    middle = []
    for row in range(count):
        entry = jnp.ones_like(gram[0][0])
        for inner in range(row):
            entry = entry - factor[row][inner] * middle[inner]
        middle.append(entry / factor[row][row])
    weights = [None] * count
    for row in range(count - 1, -1, -1):
        entry = middle[row]
        for inner in range(row + 1, count):
            entry = entry - factor[inner][row] * weights[inner]
        weights[row] = entry / factor[row][row]
    whole = weights[0]
    for row in range(1, count):
        whole = whole + weights[row]
    return [weight / whole for weight in weights]


def combine_kernel(plan, members, *refs):
    (res_ref, t_ref) = refs[:2]
    history = refs[2 : members + 2]
    (stat_ref, out_ref, weight_ref) = refs[members + 2 :]
    part = pl.program_id(0)
    block = pl.program_id(1)

    @pl.when(jnp.logical_and(part == 0, block == 0))
    def _():
        lane = lax.broadcasted_iota(jnp.int32, (8, LANES), 1)
        stats = stat_ref[...]
        gram = []
        index = 0
        for i in range(members + 1):
            row = []
            for j in range(i + 1):
                chosen = jnp.where(lane == index, stats, 0.0)
                row.append(jnp.sum(chosen, axis=1, keepdims=True))
                index += 1
            gram.append(row)
        weights = solve_weights(gram, members + 1)
        for member in range(members + 1):
            weight_ref[member] = jnp.broadcast_to(weights[member], (8, LANES))

    rows = out_ref.shape[1]
    rows = pl.ds(block * rows, rows)
    weights = [weight_ref[member, 0:1, 0:1] for member in range(members + 1)]
    value = weights[members] * (t_ref[part, rows] + MIXING * res_ref[part, rows])
    for member in range(members):
        value = value + weights[member] * history[member][part, rows]
    out_ref[0] = value


def combine_call(plan, stats, held):
    members = len(held) - 2
    like = held[-1]
    rows = plan.xblock
    return pl.pallas_call(
        functools.partial(combine_kernel, plan, members),
        grid=(plan.count, plan.rows // rows),
        in_specs=[pl.BlockSpec(memory_space=pltpu.VMEM)] * (len(held) + 1),
        out_specs=pl.BlockSpec((1, rows, plan.cols, plan.nz), lambda s, b: (s, b, 0, 0)),
        out_shape=jax.ShapeDtypeStruct(like.shape, jnp.float32),
        scratch_shapes=[pltpu.VMEM((members + 1, 8, LANES), jnp.float32)],
        compiler_params=pltpu.CompilerParams(
            dimension_semantics=("arbitrary", "arbitrary"), vmem_limit_bytes=8 * MIB
        ),
        cost_estimate=pl.CostEstimate(
            flops=10 * like.size, bytes_accessed=4 * like.size, transcendentals=0
        ),
        name="combine",
    )(*held, stats)


def hold_kernel(slots, *refs):
    sources = refs[: len(slots)]
    targets = refs[len(slots) + 1 : -1]
    sems = refs[-1]
    copies = []
    for source, slot, target in zip(sources, slots, targets):
        strip = target.shape[1] // SPLITS
        for part in range(target.shape[0]):
            place = source.at[part] if slot is None else source.at[slot, part]
            for begin in range(0, target.shape[1], strip):
                rows = pl.ds(begin, strip)
                copies.append(
                    pltpu.make_async_copy(
                        place.at[rows], target.at[part, rows], sems.at[len(copies)]
                    )
                )
    for copy in copies:
        copy.start()
    for copy in copies:
        copy.wait()


def hold_call(plan, sources, slots, shape, token):
    sources = [in_hbm(source) for source in sources]
    return pl.pallas_call(
        functools.partial(hold_kernel, slots),
        in_specs=[pl.BlockSpec(memory_space=pltpu.HBM)] * len(sources)
        + [pl.BlockSpec(memory_space=pl.ANY)],
        out_specs=[pl.BlockSpec(memory_space=pltpu.VMEM)] * len(sources),
        out_shape=[pltpu.VMEM(shape, jnp.float32)] * len(sources),
        scratch_shapes=[pltpu.SemaphoreType.DMA((len(sources) * plan.count * SPLITS,))],
        compiler_params=pltpu.CompilerParams(vmem_limit_bytes=8 * MIB),
        cost_estimate=pl.CostEstimate(
            flops=1000000, bytes_accessed=4 * len(sources) * math.prod(shape), transcendentals=0
        ),
        name="hold",
    )(*sources, token)


def exchange(array):
    return lax.all_to_all(array, BOTH, split_axis=0, concat_axis=0, tiled=True)


def in_hbm(array):
    return pltpu.with_memory_space_constraint(array, pltpu.HBM)


def add_kernel(left_ref, right_ref, *refs):
    out_ref = refs[-1]
    out_ref[...] = left_ref[...] + right_ref[...]


def add_tiles(left, right, held):
    tile = pl.BlockSpec(memory_space=pltpu.VMEM)
    return pl.pallas_call(
        add_kernel,
        in_specs=[tile, tile] + [tile] * len(held),
        out_specs=tile,
        out_shape=jax.ShapeDtypeStruct(left.shape, left.dtype),
        compiler_params=pltpu.CompilerParams(vmem_limit_bytes=MIB),
        name="add_tiles",
    )(left, right, *held)


def sum_and_hold(plan, stats, mixed_history, t_now, residual, kept):
    members = mixed_history.shape[0]
    loads = [((mixed_history,), (member,)) for member in range(members)]
    if kept is None:
        loads.insert(0, ((residual, t_now), (None, None)))
        held = []
    else:
        loads.insert(0, ((t_now,), (None,)))
        held = [kept]
    for axis, size in (("slab", plan.slabs), ("site", plan.sites)):
        if size & (size - 1):
            stats = lax.psum(stats, axis)
            continue
        hop = 1
        while hop < size:
            pairs = [(device, device ^ hop) for device in range(size)]
            arrived = lax.ppermute(stats, axis, pairs)
            now = []
            if loads:
                sources, slots = loads.pop(0)
                now = hold_call(plan, sources, slots, t_now.shape, stats)
            held.extend(now)
            stats = add_tiles(stats, arrived, now)
            hop *= 2
    for sources, slots in loads:
        held.extend(hold_call(plan, sources, slots, t_now.shape, stats))
    return stats, held


def local(plan, potential, t_now, hist_t, hist_r, chi_self, chi_cross):
    forward, inverse = plan.depth_tables()
    plane_tables = []
    for group in plan.plane_tables():
        for table in group:
            plane_tables.extend(jnp.asarray(half) for half in halves_of(table))
    constants = lambda array: [jnp.asarray(half) for half in halves_of(array)]
    early = inverse[: plan.chunks - 1].reshape(-1, plan.nz)
    shape = (plan.devices, plan.per_chunk * 2 * plan.lines, LANES)
    mixed_history, old_sums = history_call(plan, hist_t, hist_r)
    sent = []
    total = None
    for chunk in range(plan.chunks):
        table = [jnp.asarray(half) for half in halves_of(forward[chunk])]
        with_total = chunk == plan.chunks - 1
        tokens = [old_sums] if chunk else []
        outs = forward_call(plan, t_now, potential, table, with_total, tokens)
        if with_total:
            total = outs[0]
        sent.append(exchange(outs[-1].reshape(shape)))
    back = []
    for chunk in range(plan.chunks):
        planes = middle_call(plan, chunk, sent[chunk], chi_self, chi_cross, plane_tables)
        back.append(exchange(planes.reshape(shape)))
    late = constants(inverse[-1])
    if plan.chunks == 1:
        residual, stats = residual_call(plan, back, late, total, hist_r, old_sums)
        kept = None
    else:
        base, some = partial_call(plan, back[:-1], constants(early), total, hist_r)
        duals = dual_call(plan, hist_r, late)
        residual, stats, kept = final_call(plan, back[-1], late, base, duals, old_sums, some)
    stats, held = sum_and_hold(plan, stats, mixed_history, t_now, residual, kept)
    result = combine_call(plan, stats, held)
    return (result, residual)


def solution(mesh):
    def body(potential, t_now, hist_t, hist_r, chi_self, chi_cross):
        shape = (
            t_now.shape[0],
            t_now.shape[1] * mesh.shape["slab"],
            t_now.shape[2] * mesh.shape["site"],
            t_now.shape[3],
        )
        return local(Plan(mesh, shape), potential, t_now, hist_t, hist_r, chi_self, chi_cross)

    return jax.shard_map(
        body,
        mesh=mesh,
        in_specs=(
            P(None, "slab", "site", None),
            P(None, "slab", "site", None),
            P(None, None, "slab", "site", None),
            P(None, None, "slab", "site", None),
            P(None, BOTH, None, None),
            P(None, BOTH, None, None),
        ),
        out_specs=(P(None, "slab", "site", None), P(None, "slab", "site", None)),
        check_vma=False,
    )
```

```python
import functools
import math

import jax
import jax.numpy as jnp
import ml_dtypes
import numpy as np
from jax import lax
from jax.experimental import pallas as pl
from jax.experimental.pallas import tpu as pltpu
from jax.sharding import PartitionSpec as P

MIXING = 0.5
LANES = 128
BOTH = ("slab", "site")
MIB = 1024 * 1024
SPLITS = 4


def halves_of(table):
    high = table.astype(ml_dtypes.bfloat16)
    low = (table - high.astype(np.float64)).astype(ml_dtypes.bfloat16)
    return high, low


def split(values):
    high = values.astype(jnp.bfloat16)
    low = (values - high.astype(jnp.float32)).astype(jnp.bfloat16)
    return high, low


def dot3(left, right, dims):
    dot = functools.partial(
        lax.dot_general, dimension_numbers=(dims, ((), ())), preferred_element_type=jnp.float32
    )
    return dot(left[0], right[0]) + (dot(left[0], right[1]) + dot(left[1], right[0]))


NN = ((1,), (0,))
NT = ((1,), (1,))
TN = ((0,), (0,))


class Plan:
    def __init__(self, mesh, shape):
        self.slabs = mesh.shape["slab"]
        self.sites = mesh.shape["site"]
        self.devices = self.slabs * self.sites
        self.count, self.nx, self.ny, self.nz = shape
        self.rows = self.nx // self.slabs
        self.cols = self.ny // self.sites
        self.pack = LANES // self.cols
        self.planes = self.rows * self.cols // LANES
        self.half = self.nz // (2 * self.devices)
        self.chunks = 2 if self.half % 2 == 0 else 1
        self.per_chunk = self.half // self.chunks
        self.waves = self.devices * self.per_chunk * 2
        self.lines = self.count * self.planes
        self.xblock = min(self.rows, max(1, 1024 // self.cols))

    def depth_tables(self):
        z = np.arange(self.nz)
        forward = np.zeros((self.chunks, self.waves, self.nz))
        inverse = np.zeros((self.chunks, self.waves, self.nz))
        scale = 1.0 / (self.nx * self.ny * self.nz)
        alternate = 1.0 - 2.0 * (z % 2)
        for chunk in range(self.chunks):
            for device in range(self.devices):
                for j in range(self.per_chunk):
                    kz = device * self.half + chunk * self.per_chunk + j
                    row = (device * self.per_chunk + j) * 2
                    angle = 2.0 * math.pi * (kz * z % self.nz) / self.nz
                    if kz == 0:
                        forward[chunk, row] = 1.0
                        forward[chunk, row + 1] = alternate
                        inverse[chunk, row] = scale
                        inverse[chunk, row + 1] = scale * alternate
                    else:
                        forward[chunk, row] = np.cos(angle)
                        forward[chunk, row + 1] = -np.sin(angle)
                        inverse[chunk, row] = 2.0 * scale * np.cos(angle)
                        inverse[chunk, row + 1] = -2.0 * scale * np.sin(angle)
        return forward, inverse

    def plane_tables(self):
        index = np.arange(self.ny)
        angle = 2.0 * math.pi * (index[:, None] * index[None, :] % self.ny) / self.ny
        second = [np.cos(angle), np.sin(angle)]
        low, slab, plane = np.meshgrid(
            np.arange(self.pack), np.arange(self.slabs), np.arange(self.planes), indexing="ij"
        )
        order = (slab * self.rows + plane * self.pack + low).reshape(-1)
        waves = np.arange(self.nx)
        angle = 2.0 * math.pi * (waves[:, None] * order[None, :] % self.nx) / self.nx
        first = [np.cos(angle), np.sin(angle)]
        return second, first, [first[0].T, first[1].T]


def total_of(indirect, potential):
    field_value = indirect - potential
    near = field_value + field_value * field_value * (0.5 + field_value * (1.0 / 6.0))
    growth = jnp.where(field_value > -0.01, near, jnp.exp(field_value) - 1.0)
    return jnp.where(field_value > 0, field_value, growth)


def forward_kernel(plan, with_total, t_ref, pot_ref, high_ref, low_ref, *refs):
    outs = refs[-2:] if with_total else refs[-1:]
    out_ref = outs[-1]
    part = pl.program_id(0)
    block = pl.program_id(1)
    size = plan.xblock * plan.cols
    indirect = t_ref[0].reshape(size, plan.nz)
    total = total_of(indirect, pot_ref[0].reshape(size, plan.nz))
    if with_total:
        outs[0][0] = total.reshape(plan.xblock, plan.cols, plan.nz)
    direct = split(total - indirect)
    result = dot3(direct, (high_ref[...], low_ref[...]), NN)
    count = size // LANES
    for index in range(count):
        line = part * plan.planes + block * count + index
        out_ref[pl.ds(line, plan.waves, stride=plan.lines), :] = result[
            index * LANES : (index + 1) * LANES
        ].T


def forward_call(plan, t_now, potential, table, with_total, tokens):
    blocks = plan.rows // plan.xblock
    field_spec = pl.BlockSpec(
        (1, plan.xblock, plan.cols, plan.nz), lambda s, b: (s, b, 0, 0)
    )
    table_spec = pl.BlockSpec((plan.nz, plan.waves), lambda s, b: (0, 0))
    rows = plan.waves * plan.lines
    out_specs = [pl.BlockSpec((rows, LANES), lambda s, b: (0, 0))]
    out_shape = [jax.ShapeDtypeStruct((rows, LANES), jnp.float32)]
    if with_total:
        out_specs = [field_spec] + out_specs
        out_shape = [jax.ShapeDtypeStruct(t_now.shape, jnp.float32)] + out_shape
    return pl.pallas_call(
        functools.partial(forward_kernel, plan, with_total),
        grid=(plan.count, blocks),
        in_specs=[field_spec, field_spec, table_spec, table_spec]
        + [pl.BlockSpec(memory_space=pl.ANY)] * len(tokens),
        out_specs=out_specs,
        out_shape=out_shape,
        compiler_params=pltpu.CompilerParams(
            dimension_semantics=("arbitrary", "arbitrary"), vmem_limit_bytes=56 * MIB
        ),
        cost_estimate=pl.CostEstimate(
            flops=2 * 3 * t_now.size * plan.waves,
            bytes_accessed=12 * t_now.size,
            transcendentals=t_now.size,
        ),
        name="forward_depth",
    )(t_now, potential, *table, *tokens)


def middle_kernel(
    plan, first_chunk, in_ref, self_ref, cross_ref, self_top, cross_top, *refs
):
    (tables, rest) = (refs[:12], refs[12:])
    (out_ref, wide, mixed, chi, second) = rest
    step = pl.program_id(0)
    span = plan.slabs * plan.planes
    depth = plan.sites * LANES
    nx, ny = plan.nx, plan.ny
    cols = plan.cols

    @pl.when(step == 0)
    def _():
        second[...] = jnp.zeros_like(second)
        for index in range(4):
            for low in range(plan.pack):
                for site in range(plan.sites):
                    base = site * LANES + low * cols
                    second[index, base : base + cols, low * ny : (low + 1) * ny] = tables[index][
                        site * cols : (site + 1) * cols, :
                    ]

    first_device = jnp.logical_and(lax.axis_index("slab") == 0, lax.axis_index("site") == 0)
    special = jnp.logical_and(first_device, step == 0) if first_chunk else None
    passes = jnp.where(special, 2, 1) if first_chunk else 1

    aligned = plan.planes % 8 == 0

    def repeat(body):
        if aligned:
            lax.fori_loop(0, plan.count, body, 0)
        else:
            for part in range(plan.count):
                body(part, 0)

    def gather(part, imaginary):
        base = (imaginary * plan.count + part) * plan.planes
        base = pl.multiple_of(base, 8) if aligned else base
        pieces = []
        for site in range(plan.sites):
            if aligned:
                piece = in_ref[:, site, 0, pl.ds(base, plan.planes), :].reshape(span, LANES)
            else:
                piece = jnp.concatenate(
                    [
                        in_ref[slab, site, 0, base : base + plan.planes, :]
                        for slab in range(plan.slabs)
                    ],
                    axis=0,
                )
            pieces.append(piece)
        return jnp.concatenate(pieces, axis=1)

    def scatter(part, imaginary, values):
        base = (imaginary * plan.count + part) * plan.planes
        base = pl.multiple_of(base, 8) if aligned else base
        for site in range(plan.sites):
            piece = values[:, site * LANES : (site + 1) * LANES]
            if aligned:
                out_ref[:, site, 0, pl.ds(base, plan.planes), :] = piece.reshape(
                    plan.slabs, plan.planes, LANES
                )
            else:
                for slab in range(plan.slabs):
                    out_ref[slab, site, 0, base : base + plan.planes, :] = piece[
                        slab * plan.planes : (slab + 1) * plan.planes
                    ]

    def run(turn, carry):
        for index in range(plan.count):
            low_self = self_ref[index, 0]
            low_cross = cross_ref[index, 0]
            if first_chunk:
                use_top = turn == 1
                low_self = jnp.where(use_top, self_top[index, 0], low_self)
                low_cross = jnp.where(use_top, cross_top[index, 0], low_cross)
            chi[index] = low_self.T
            chi[plan.count + index] = low_cross.T
        cos_second = (second[0], second[1])
        sin_second = (second[2], second[3])
        cos_first = (tables[4][...], tables[5][...])
        sin_first = (tables[6][...], tables[7][...])
        cos_back = (tables[8][...], tables[9][...])
        sin_back = (tables[10][...], tables[11][...])
        def forward(part, carry):
            real = gather(part, 0)
            imag = gather(part, 1)
            if first_chunk:
                real, imag = (
                    jnp.where(turn == 1, imag, real),
                    jnp.where(special, 0.0, imag),
                )
            real, imag = split(real), split(imag)
            new_real = dot3(real, cos_second, NN) + dot3(imag, sin_second, NN)
            new_imag = dot3(imag, cos_second, NN) - dot3(real, sin_second, NN)
            for low in range(plan.pack):
                wide[low * span : (low + 1) * span, :ny] = new_real[:, low * ny : (low + 1) * ny]
                wide[low * span : (low + 1) * span, ny:] = new_imag[:, low * ny : (low + 1) * ny]
            both = split(wide[...])
            by_cos = dot3(cos_first, both, NN)
            by_sin = dot3(sin_first, both, NN)
            mixed[part, :, :ny] = by_cos[:, :ny] + by_sin[:, ny:]
            mixed[part, :, ny:] = by_cos[:, ny:] - by_sin[:, :ny]
            return carry

        repeat(forward)
        cross_at = {(0, 1): 0, (0, 2): 1, (1, 2): 2}
        strip = 32

        @pl.loop(0, nx // strip)
        def _(index):
            rows = pl.ds(pl.multiple_of(index * strip, strip), strip)
            loaded = [chi[index, rows, :] for index in range(2 * plan.count)]
            for side in range(2):
                lanes = pl.ds(side * ny, ny)
                fields = [mixed[part, rows, lanes] for part in range(plan.count)]
                for part in range(plan.count):
                    value = loaded[part] * fields[part]
                    for other in range(plan.count):
                        if other != part:
                            pair = cross_at[(min(part, other), max(part, other))]
                            value = value + loaded[plan.count + pair] * fields[other]
                    mixed[part, rows, lanes] = value
        def inverse(part, carry):
            both = split(mixed[part])
            by_cos = dot3(cos_back, both, NN)
            by_sin = dot3(sin_back, both, NN)
            real = split(by_cos[:, :ny] - by_sin[:, ny:])
            imag = split(by_cos[:, ny:] + by_sin[:, :ny])
            new_real = None
            new_imag = None
            for low in range(plan.pack):
                rows = slice(low * span, (low + 1) * span)
                lanes = slice(low * ny, (low + 1) * ny)
                cosine = (second[0, :, lanes], second[1, :, lanes])
                sine = (second[2, :, lanes], second[3, :, lanes])
                some_real = (real[0][rows], real[1][rows])
                some_imag = (imag[0][rows], imag[1][rows])
                add_real = dot3(some_real, cosine, NT) - dot3(some_imag, sine, NT)
                add_imag = dot3(some_imag, cosine, NT) + dot3(some_real, sine, NT)
                new_real = add_real if new_real is None else new_real + add_real
                new_imag = add_imag if new_imag is None else new_imag + add_imag
            if first_chunk:

                @pl.when(turn == 0)
                def _(part=part, new_real=new_real):
                    scatter(part, 0, new_real)

                @pl.when(jnp.logical_or(turn == 1, jnp.logical_not(special)))
                def _(part=part, new_real=new_real, new_imag=new_imag):
                    scatter(part, 1, jnp.where(special, new_real, new_imag))
            else:
                scatter(part, 0, new_real)
                scatter(part, 1, new_imag)
            return carry

        repeat(inverse)
        return carry

    if first_chunk:
        lax.fori_loop(0, passes, run, 0)
    else:
        run(0, 0)


def middle_call(plan, chunk, piece, chi_self, chi_cross, tables):
    shape = (plan.slabs, plan.sites, plan.per_chunk, 2 * plan.lines, LANES)
    piece = piece.reshape(shape)
    if chunk < plan.chunks - 1:
        piece = pltpu.with_memory_space_constraint(piece, pltpu.VMEM)
    data_spec = pl.BlockSpec(
        (plan.slabs, plan.sites, 1, 2 * plan.lines, LANES), lambda j: (0, 0, j, 0, 0)
    )
    base = chunk * plan.per_chunk
    row_spec = pl.BlockSpec((plan.count, 1, plan.ny, plan.nx), lambda j: (0, base + j, 0, 0))
    top_spec = pl.BlockSpec((plan.count, 1, plan.ny, plan.nx), lambda j: (0, plan.half, 0, 0))
    table_specs = [pl.BlockSpec(table.shape, lambda j: (0, 0)) for table in tables]
    depth = plan.sites * LANES
    flops = 2 * 3 * 2 * plan.count * 4 * plan.per_chunk * plan.nx * plan.ny * (plan.nx + depth)
    return pl.pallas_call(
        functools.partial(middle_kernel, plan, chunk == 0),
        grid=(plan.per_chunk,),
        in_specs=[data_spec, row_spec, row_spec, top_spec, top_spec]
        + table_specs,
        out_specs=data_spec,
        out_shape=jax.ShapeDtypeStruct(shape, jnp.float32),
        scratch_shapes=[
            pltpu.VMEM((plan.nx, 2 * plan.ny), jnp.float32),
            pltpu.VMEM((plan.count, plan.nx, 2 * plan.ny), jnp.float32),
            pltpu.VMEM((2 * plan.count, plan.nx, plan.ny), jnp.float32),
            pltpu.VMEM((4, depth, plan.pack * plan.ny), jnp.bfloat16),
        ],
        compiler_params=pltpu.CompilerParams(
            dimension_semantics=("arbitrary",), vmem_limit_bytes=56 * MIB
        ),
        cost_estimate=pl.CostEstimate(
            flops=flops, bytes_accessed=4 * piece.size * 4, transcendentals=0
        ),
        name="middle_planes",
    )(piece, chi_self, chi_cross, chi_self, chi_cross, *tables)


def fold(values):
    return jnp.sum(values.reshape(-1, 8, values.shape[-1]), axis=0)


def history_kernel(plan, members, t_ref, r_ref, u_ref, sum_ref):
    first = jnp.logical_and(pl.program_id(0) == 0, pl.program_id(1) == 0)

    @pl.when(first)
    def _():
        sum_ref[...] = jnp.zeros_like(sum_ref)

    residuals = [r_ref[member, 0] for member in range(members)]
    for member in range(members):
        u_ref[member, 0] = t_ref[member, 0] + MIXING * residuals[member]
    index = 0
    for i in range(members):
        for j in range(i + 1):
            sum_ref[index] += fold(residuals[i] * residuals[j])
            index += 1


def history_call(plan, hist_t, hist_r):
    members = hist_t.shape[0]
    block = (members, 1, min(plan.xblock, 4), plan.cols, plan.nz)
    spec = pl.BlockSpec(block, lambda s, b: (0, s, b, 0, 0))
    pairs = members * (members + 1) // 2
    sum_spec = pl.BlockSpec((pairs, 8, plan.nz), lambda s, b: (0, 0, 0))
    return pl.pallas_call(
        functools.partial(history_kernel, plan, members),
        grid=(plan.count, plan.rows // block[2]),
        in_specs=[spec, spec],
        out_specs=[spec, sum_spec],
        out_shape=[
            pltpu.HBM(hist_t.shape, jnp.float32),
            jax.ShapeDtypeStruct((pairs, 8, plan.nz), jnp.float32),
        ],
        compiler_params=pltpu.CompilerParams(
            dimension_semantics=("arbitrary", "arbitrary"), vmem_limit_bytes=56 * MIB
        ),
        cost_estimate=pl.CostEstimate(
            flops=50 * hist_t.size, bytes_accessed=12 * hist_t.size, transcendentals=0
        ),
        name="history",
    )(hist_t, hist_r)


def residual_kernel(plan, members, *refs):
    pieces = refs[: plan.chunks]
    (high_ref, low_ref, total_ref, r_ref, old_ref, out_ref, stat_ref, acc) = refs[plan.chunks :]
    part = pl.program_id(0)
    block = pl.program_id(1)
    first = jnp.logical_and(part == 0, block == 0)
    last = jnp.logical_and(part == pl.num_programs(0) - 1, block == pl.num_programs(1) - 1)

    @pl.when(first)
    def _():
        acc[...] = jnp.zeros_like(acc)

    size = plan.xblock * plan.cols
    count = size // LANES
    for index in range(count):
        line = part * plan.planes + block * count + index
        gathered = jnp.concatenate(
            [piece[pl.ds(line, plan.waves, stride=plan.lines), :] for piece in pieces], axis=0
        )
        turned = split(gathered.T)
        field = dot3(turned, (high_ref[...], low_ref[...]), NN)
        rows = pl.ds(index * plan.pack, plan.pack)
        field = field.reshape(plan.pack, plan.cols, plan.nz) - total_ref[0, rows]
        out_ref[0, rows] = field
        for member in range(members):
            acc[member] += fold(field * r_ref[member, 0, rows])
        acc[members] += fold(field * field)

    @pl.when(last)
    def _():
        lane = lax.broadcasted_iota(jnp.int32, (8, LANES), 1)
        stats = jnp.zeros((8, LANES), jnp.float32)
        pairs = members * (members + 1) // 2
        for index in range(pairs + members + 1):
            tile = old_ref[index] if index < pairs else acc[index - pairs]
            stats = jnp.where(lane == index, jnp.sum(tile), stats)
        stat_ref[...] = stats


def residual_call(plan, pieces, table, total, hist_r, old_sums):
    members = hist_r.shape[0]
    rows = plan.waves * plan.lines
    pieces = [in_hbm(piece.reshape(rows, LANES)) for piece in pieces]
    spec = pl.BlockSpec((1, plan.xblock, plan.cols, plan.nz), lambda s, b: (s, b, 0, 0))
    hist_spec = pl.BlockSpec(
        (members, 1, plan.xblock, plan.cols, plan.nz), lambda s, b: (0, s, b, 0, 0)
    )
    whole = lambda array: pl.BlockSpec(array.shape, lambda s, b: (0,) * array.ndim)
    return pl.pallas_call(
        functools.partial(residual_kernel, plan, members),
        grid=(plan.count, plan.rows // plan.xblock),
        in_specs=[whole(piece) for piece in pieces]
        + [whole(table[0]), whole(table[1]), spec, hist_spec, whole(old_sums)],
        out_specs=[spec, pl.BlockSpec((8, LANES), lambda s, b: (0, 0))],
        out_shape=[
            pltpu.HBM(total.shape, jnp.float32),
            jax.ShapeDtypeStruct((8, LANES), jnp.float32),
        ],
        scratch_shapes=[pltpu.VMEM((members + 1, 8, plan.nz), jnp.float32)],
        compiler_params=pltpu.CompilerParams(
            dimension_semantics=("arbitrary", "arbitrary"), vmem_limit_bytes=56 * MIB
        ),
        cost_estimate=pl.CostEstimate(
            flops=2 * 3 * total.size * plan.nz,
            bytes_accessed=4 * total.size * (3 + members),
            transcendentals=0,
        ),
        name="residual",
    )(*pieces, *table, total, hist_r, old_sums)


def dual_kernel(plan, r_ref, high_ref, low_ref, out_ref):
    part = pl.program_id(1)
    block = pl.program_id(2)
    size = plan.xblock * plan.cols
    values = split(r_ref[0, 0].reshape(size, plan.nz))
    result = dot3(values, (high_ref[...], low_ref[...]), NN)
    count = size // LANES
    for index in range(count):
        line = part * plan.planes + block * count + index
        out_ref[0, pl.ds(line, plan.waves, stride=plan.lines), :] = result[
            index * LANES : (index + 1) * LANES
        ].T


def dual_call(plan, hist_r, table):
    members = hist_r.shape[0]
    rows = plan.waves * plan.lines
    spec = pl.BlockSpec(
        (1, 1, plan.xblock, plan.cols, plan.nz), lambda m, s, b: (m, s, b, 0, 0)
    )
    table_spec = pl.BlockSpec((plan.nz, plan.waves), lambda m, s, b: (0, 0))
    return pl.pallas_call(
        functools.partial(dual_kernel, plan),
        grid=(members, plan.count, plan.rows // plan.xblock),
        in_specs=[spec, table_spec, table_spec],
        out_specs=pl.BlockSpec((1, rows, LANES), lambda m, s, b: (m, 0, 0)),
        out_shape=jax.ShapeDtypeStruct((members, rows, LANES), jnp.float32),
        compiler_params=pltpu.CompilerParams(
            dimension_semantics=("arbitrary",) * 3, vmem_limit_bytes=56 * MIB
        ),
        cost_estimate=pl.CostEstimate(
            flops=2 * 3 * hist_r.size * plan.waves,
            bytes_accessed=6 * hist_r.size,
            transcendentals=0,
        ),
        name="dual",
    )(hist_r, *table)


def partial_kernel(plan, members, *refs):
    pieces = refs[: plan.chunks - 1]
    (high_ref, low_ref, total_ref, r_ref, out_ref, acc) = refs[plan.chunks - 1 :]
    part = pl.program_id(0)
    block = pl.program_id(1)

    @pl.when(jnp.logical_and(part == 0, block == 0))
    def _():
        acc[...] = jnp.zeros_like(acc)

    field = piece_field(plan, pieces, high_ref, low_ref) - total_ref[0]
    out_ref[0] = field
    for member in range(members):
        acc[member] += fold(field * r_ref[member, 0])


def piece_field(plan, pieces, high_ref, low_ref):
    count = plan.xblock * plan.cols // LANES
    turned = []
    for index in range(count):
        line = pl.program_id(0) * plan.planes + pl.program_id(1) * count + index
        gathered = [piece[pl.ds(line, plan.waves, stride=plan.lines), :] for piece in pieces]
        gathered = gathered[0] if len(gathered) == 1 else jnp.concatenate(gathered, axis=0)
        turned.append(gathered.T)
    field = dot3(split(jnp.concatenate(turned, axis=0)), (high_ref[...], low_ref[...]), NN)
    return field.reshape(plan.xblock, plan.cols, plan.nz)


def partial_call(plan, pieces, table, total, hist_r):
    members = hist_r.shape[0]
    rows = plan.waves * plan.lines
    pieces = [in_hbm(piece.reshape(rows, LANES)) for piece in pieces]
    spec = pl.BlockSpec((1, plan.xblock, plan.cols, plan.nz), lambda s, b: (s, b, 0, 0))
    hist_spec = pl.BlockSpec(
        (members, 1, plan.xblock, plan.cols, plan.nz), lambda s, b: (0, s, b, 0, 0)
    )
    whole = lambda array: pl.BlockSpec(array.shape, lambda s, b: (0,) * array.ndim)
    return pl.pallas_call(
        functools.partial(partial_kernel, plan, members),
        grid=(plan.count, plan.rows // plan.xblock),
        in_specs=[whole(array) for array in (*pieces, *table)] + [spec, hist_spec],
        out_specs=[spec, pl.BlockSpec((members, 8, plan.nz), lambda s, b: (0, 0, 0))],
        out_shape=[
            jax.ShapeDtypeStruct(total.shape, jnp.float32),
            jax.ShapeDtypeStruct((members, 8, plan.nz), jnp.float32),
        ],
        compiler_params=pltpu.CompilerParams(
            dimension_semantics=("arbitrary", "arbitrary"), vmem_limit_bytes=56 * MIB
        ),
        cost_estimate=pl.CostEstimate(
            flops=2 * 3 * total.size * plan.nz,
            bytes_accessed=4 * total.size * (3 + members),
            transcendentals=0,
        ),
        name="partial",
    )(*pieces, *table, total, hist_r)


def final_kernel(plan, members, *refs):
    (piece_ref, high_ref, low_ref, base_ref, dual_ref, old_ref, some_ref) = refs[:7]
    (stat_ref, keep_ref, acc, square) = refs[7:]
    part = pl.program_id(0)
    block = pl.program_id(1)
    blocks = pl.num_programs(1)
    first = jnp.logical_and(part == 0, block == 0)
    last = jnp.logical_and(part == pl.num_programs(0) - 1, block == blocks - 1)

    @pl.when(first)
    def _():
        acc[...] = jnp.zeros_like(acc)
        square[...] = jnp.zeros_like(square)

    share = dual_ref.shape[1]
    start = pl.multiple_of((part * blocks + block) * share, share)
    waves = piece_ref[pl.ds(start, share), :]
    for member in range(members):
        acc[member] += fold(waves * dual_ref[member])
    field = piece_field(plan, [piece_ref], high_ref, low_ref) + base_ref[0]
    keep_ref[part, pl.ds(block * plan.xblock, plan.xblock)] = field
    square[...] += fold(field * field)

    @pl.when(last)
    def _():
        lane = lax.broadcasted_iota(jnp.int32, (8, LANES), 1)
        stats = jnp.zeros((8, LANES), jnp.float32)
        pairs = members * (members + 1) // 2
        for index in range(pairs):
            stats = jnp.where(lane == index, jnp.sum(old_ref[index]), stats)
        for member in range(members):
            value = jnp.sum(some_ref[member]) + jnp.sum(acc[member])
            stats = jnp.where(lane == pairs + member, value, stats)
        stats = jnp.where(lane == pairs + members, jnp.sum(square[...]), stats)
        stat_ref[...] = stats


def final_call(plan, piece, table, base, duals, old_sums, some_sums):
    members = duals.shape[0]
    rows = plan.waves * plan.lines
    piece = in_hbm(piece.reshape(rows, LANES))
    blocks = plan.rows // plan.xblock
    share = rows // (plan.count * blocks)
    spec = pl.BlockSpec((1, plan.xblock, plan.cols, plan.nz), lambda s, b: (s, b, 0, 0))
    dual_spec = pl.BlockSpec((members, share, LANES), lambda s, b: (0, s * blocks + b, 0))
    whole = lambda array: pl.BlockSpec(array.shape, lambda s, b: (0,) * array.ndim)
    return pl.pallas_call(
        functools.partial(final_kernel, plan, members),
        grid=(plan.count, blocks),
        in_specs=[whole(piece), whole(table[0]), whole(table[1]), spec, dual_spec]
        + [whole(old_sums), whole(some_sums)],
        out_specs=[
            pl.BlockSpec((8, LANES), lambda s, b: (0, 0)),
            pl.BlockSpec(memory_space=pltpu.VMEM),
        ],
        out_shape=[
            pltpu.VMEM((8, LANES), jnp.float32),
            pltpu.VMEM(base.shape, jnp.float32),
        ],
        scratch_shapes=[
            pltpu.VMEM((members, 8, LANES), jnp.float32),
            pltpu.VMEM((8, plan.nz), jnp.float32),
        ],
        compiler_params=pltpu.CompilerParams(
            dimension_semantics=("arbitrary", "arbitrary"), vmem_limit_bytes=50 * MIB
        ),
        cost_estimate=pl.CostEstimate(
            flops=2 * 3 * base.size * plan.waves,
            bytes_accessed=4 * base.size * 5,
            transcendentals=0,
        ),
        name="final",
    )(piece, *table, base, duals, old_sums, some_sums)


def solve_weights(gram, count):
    factor = [[None] * count for member in range(count)]
    for column in range(count):
        diagonal_sum = gram[column][column]
        for inner in range(column):
            diagonal_sum = diagonal_sum - factor[column][inner] * factor[column][inner]
        factor[column][column] = jnp.sqrt(diagonal_sum)
        for row in range(column + 1, count):
            entry = gram[row][column]
            for inner in range(column):
                entry = entry - factor[row][inner] * factor[column][inner]
            factor[row][column] = entry / factor[column][column]
    middle = []
    for row in range(count):
        entry = jnp.ones_like(gram[0][0])
        for inner in range(row):
            entry = entry - factor[row][inner] * middle[inner]
        middle.append(entry / factor[row][row])
    weights = [None] * count
    for row in range(count - 1, -1, -1):
        entry = middle[row]
        for inner in range(row + 1, count):
            entry = entry - factor[inner][row] * weights[inner]
        weights[row] = entry / factor[row][row]
    whole = weights[0]
    for row in range(1, count):
        whole = whole + weights[row]
    return [weight / whole for weight in weights]


def combine_kernel(plan, members, *refs):
    newest = refs[0]
    history = [refs[1], *refs[3 : members + 2]]
    t_ref = refs[2]
    (stat_ref, out_ref, weight_ref) = refs[members + 2 :]
    part = pl.program_id(0)
    block = pl.program_id(1)

    @pl.when(jnp.logical_and(part == 0, block == 0))
    def _():
        lane = lax.broadcasted_iota(jnp.int32, (8, LANES), 1)
        stats = stat_ref[...]
        gram = []
        index = 0
        for i in range(members + 1):
            row = []
            for j in range(i + 1):
                chosen = jnp.where(lane == index, stats, 0.0)
                row.append(jnp.sum(chosen, axis=1, keepdims=True))
                index += 1
            gram.append(row)
        weights = solve_weights(gram, members + 1)
        for member in range(members + 1):
            weight_ref[member] = jnp.broadcast_to(weights[member], (8, LANES))

    rows = out_ref.shape[1]
    rows = pl.ds(block * rows, rows)
    weights = [weight_ref[member, 0:1, 0:1] for member in range(members + 1)]
    value = weights[members] * (t_ref[part, rows] + MIXING * newest[part, rows])
    for member in range(members):
        value = value + weights[member] * history[member][part, rows]
    out_ref[0] = value


def combine_call(plan, stats, held):
    members = len(held) - 2
    like = held[0]
    rows = plan.xblock
    spec = pl.BlockSpec((1, rows, plan.cols, plan.nz), lambda s, b: (s, b, 0, 0))
    return pl.pallas_call(
        functools.partial(combine_kernel, plan, members),
        grid=(plan.count, plan.rows // rows),
        in_specs=[pl.BlockSpec(memory_space=pltpu.VMEM)] * (len(held) + 1),
        out_specs=spec,
        out_shape=jax.ShapeDtypeStruct(like.shape, jnp.float32),
        scratch_shapes=[pltpu.VMEM((members + 1, 8, LANES), jnp.float32)],
        compiler_params=pltpu.CompilerParams(
            dimension_semantics=("arbitrary", "arbitrary"), vmem_limit_bytes=8 * MIB
        ),
        cost_estimate=pl.CostEstimate(
            flops=10 * like.size, bytes_accessed=4 * like.size, transcendentals=0
        ),
        name="combine",
    )(*held, stats)


def hold_kernel(slots, *refs):
    sources = refs[: len(slots)]
    targets = refs[len(slots) + 1 : -1]
    sems = refs[-1]
    copies = []
    for source, slot, target in zip(sources, slots, targets):
        strip = target.shape[1] // SPLITS
        for part in range(target.shape[0]):
            place = source.at[part] if slot is None else source.at[slot, part]
            for begin in range(0, target.shape[1], strip):
                rows = pl.ds(begin, strip)
                copies.append(
                    pltpu.make_async_copy(
                        place.at[rows], target.at[part, rows], sems.at[len(copies)]
                    )
                )
    for copy in copies:
        copy.start()
    for copy in copies:
        copy.wait()


def hold_call(plan, sources, slots, shape, token):
    sources = [in_hbm(source) for source in sources]
    return pl.pallas_call(
        functools.partial(hold_kernel, slots),
        in_specs=[pl.BlockSpec(memory_space=pltpu.HBM)] * len(sources)
        + [pl.BlockSpec(memory_space=pl.ANY)],
        out_specs=[pl.BlockSpec(memory_space=pltpu.VMEM)] * len(sources),
        out_shape=[pltpu.VMEM(shape, jnp.float32)] * len(sources),
        scratch_shapes=[pltpu.SemaphoreType.DMA((len(sources) * plan.count * SPLITS,))],
        compiler_params=pltpu.CompilerParams(vmem_limit_bytes=8 * MIB),
        cost_estimate=pl.CostEstimate(
            flops=1000000, bytes_accessed=4 * len(sources) * math.prod(shape), transcendentals=0
        ),
        name="hold",
    )(*sources, token)


def exchange(array):
    return lax.all_to_all(array, BOTH, split_axis=0, concat_axis=0, tiled=True)


def in_hbm(array):
    return pltpu.with_memory_space_constraint(array, pltpu.HBM)


def add_kernel(left_ref, right_ref, *refs):
    out_ref = refs[-1]
    out_ref[...] = left_ref[...] + right_ref[...]


def add_tiles(left, right, held):
    tile = pl.BlockSpec(memory_space=pltpu.VMEM)
    return pl.pallas_call(
        add_kernel,
        in_specs=[tile, tile] + [pl.BlockSpec(memory_space=pl.ANY)] * len(held),
        out_specs=tile,
        out_shape=jax.ShapeDtypeStruct(left.shape, left.dtype),
        compiler_params=pltpu.CompilerParams(vmem_limit_bytes=MIB),
        name="add_tiles",
    )(left, right, *held)


def drain_kernel(held_ref, token_ref, out_ref, sems):
    del token_ref
    copies = []
    strip = held_ref.shape[1] // SPLITS
    for part in range(held_ref.shape[0]):
        for begin in range(0, held_ref.shape[1], strip):
            rows = pl.ds(begin, strip)
            copies.append(
                pltpu.make_async_copy(
                    held_ref.at[part, rows], out_ref.at[part, rows], sems.at[len(copies)]
                )
            )
    for copy in copies:
        copy.start()
    for copy in copies:
        copy.wait()


def drain_call(plan, held, token):
    return pl.pallas_call(
        drain_kernel,
        in_specs=[pl.BlockSpec(memory_space=pltpu.VMEM), pl.BlockSpec(memory_space=pl.ANY)],
        out_specs=pl.BlockSpec(memory_space=pltpu.HBM),
        out_shape=jax.ShapeDtypeStruct(held.shape, jnp.float32),
        scratch_shapes=[pltpu.SemaphoreType.DMA((plan.count * SPLITS,))],
        compiler_params=pltpu.CompilerParams(vmem_limit_bytes=8 * MIB),
        cost_estimate=pl.CostEstimate(
            flops=1000000, bytes_accessed=4 * held.size, transcendentals=0
        ),
        name="drain",
    )(held, token)


def sum_and_hold(plan, stats, mixed_history, t_now, residual, kept):
    members = mixed_history.shape[0]
    shape = mixed_history.shape[1:]
    works = []
    if kept is None:
        works.append(lambda token: hold_call(plan, (residual,), (None,), shape, token))
    else:
        works.append(lambda token: [drain_call(plan, kept, token)])
    for member in range(members):
        works.append(
            lambda token, member=member: hold_call(
                plan, (mixed_history,), (member,), shape, token
            )
        )
    works[1] = lambda token: hold_call(plan, (mixed_history, t_now), (0, None), shape, token)
    done = []
    for axis, size in (("slab", plan.slabs), ("site", plan.sites)):
        if size & (size - 1):
            stats = lax.psum(stats, axis)
            continue
        hop = 1
        while hop < size:
            pairs = [(device, device ^ hop) for device in range(size)]
            arrived = lax.ppermute(stats, axis, pairs)
            now = works.pop(0)(stats) if works else []
            after = now if kept is None or done else [in_hbm(array) for array in now]
            done.extend(now)
            stats = add_tiles(stats, arrived, after)
            hop *= 2
    for work in works:
        done.extend(work(stats))
    if kept is not None:
        residual = done[0]
        done[0] = kept
    return stats, done, residual


def local(plan, potential, t_now, hist_t, hist_r, chi_self, chi_cross):
    forward, inverse = plan.depth_tables()
    plane_tables = []
    for group in plan.plane_tables():
        for table in group:
            plane_tables.extend(jnp.asarray(half) for half in halves_of(table))
    constants = lambda array: [jnp.asarray(half) for half in halves_of(array)]
    early = inverse[: plan.chunks - 1].reshape(-1, plan.nz)
    shape = (plan.devices, plan.per_chunk * 2 * plan.lines, LANES)
    mixed_history, old_sums = history_call(plan, hist_t, hist_r)
    sent = []
    total = None
    for chunk in range(plan.chunks):
        table = [jnp.asarray(half) for half in halves_of(forward[chunk].T)]
        with_total = chunk == plan.chunks - 1
        tokens = [old_sums] if chunk else []
        outs = forward_call(plan, t_now, potential, table, with_total, tokens)
        if with_total:
            total = outs[0]
        sent.append(exchange(outs[-1].reshape(shape)))
    back = []
    for chunk in range(plan.chunks):
        planes = middle_call(plan, chunk, sent[chunk], chi_self, chi_cross, plane_tables)
        back.append(exchange(planes.reshape(shape)))
    late = constants(inverse[-1])
    if plan.chunks == 1:
        residual, stats = residual_call(plan, back, late, total, hist_r, old_sums)
        kept = None
    else:
        residual = None
        base, some = partial_call(plan, back[:-1], constants(early), total, hist_r)
        duals = dual_call(plan, hist_r, constants(inverse[-1].T))
        stats, kept = final_call(plan, back[-1], late, base, duals, old_sums, some)
    stats, held, residual = sum_and_hold(plan, stats, mixed_history, t_now, residual, kept)
    result = combine_call(plan, stats, held)
    return (result, residual)


def solution(mesh):
    def body(potential, t_now, hist_t, hist_r, chi_self, chi_cross):
        shape = (
            t_now.shape[0],
            t_now.shape[1] * mesh.shape["slab"],
            t_now.shape[2] * mesh.shape["site"],
            t_now.shape[3],
        )
        return local(Plan(mesh, shape), potential, t_now, hist_t, hist_r, chi_self, chi_cross)

    return jax.shard_map(
        body,
        mesh=mesh,
        in_specs=(
            P(None, "slab", "site", None),
            P(None, "slab", "site", None),
            P(None, None, "slab", "site", None),
            P(None, None, "slab", "site", None),
            P(None, BOTH, None, None),
            P(None, BOTH, None, None),
        ),
        out_specs=(P(None, "slab", "site", None), P(None, "slab", "site", None)),
        check_vma=False,
    )
```
